32 devices in a mesh: groups: 2 (over x), ctx: 16 (over z, y, core).
Axes of the slice: x: 2, y: 2, z: 4, core: 2. Of those that a mesh axis runs over, the one named last changes fastest.
Arguments:
- queries: bfloat16 [96, 4096], P(('groups', 'ctx')), parts along dimension 0, may hold values from -200 to 200
- cache_keys: bfloat16 [4096, 512], P(('groups', 'ctx')), parts along dimension 0, may hold values from -6 to 6
- cache_values: bfloat16 [4096, 512], P(('groups', 'ctx')), parts along dimension 0, may hold values from -6 to 6
- new_keys: bfloat16 [96, 512], P(('groups', 'ctx')), parts along dimension 0, may hold values from -6 to 6
- new_values: bfloat16 [96, 512], P(('groups', 'ctx')), parts along dimension 0, may hold values from -6 to 6
- cache_lengths: int32 [32], P(('groups', 'ctx')), parts along dimension 0, may hold values from 0 to 128, as said below
- residual_in: bfloat16 [96, 2048], P(('groups', 'ctx')), parts along dimension 0, may hold values from -6 to 6
- out_weight: bfloat16 [4096, 2048], P('ctx'), may hold values from -3 to 3
- norm_gain: bfloat16 [2048], replicated, may hold values from 0.25 to 1.75
- expert_gate: bfloat16 [16, 2048, 768], P('ctx'), may hold values from -0.125 to 0.125
- expert_up: bfloat16 [16, 2048, 768], P('ctx'), may hold values from -0.125 to 0.125
- expert_down: bfloat16 [16, 768, 2048], P('ctx'), may hold values from -0.21875 to 0.21875
- expert_ids: int32 [96, 8], P(('groups', 'ctx')), parts along dimension 0, may hold values from 0 to 15, all different within a row; in each aligned block of 3 rows (0 to 2, 3 to 5, ...) at most 3 rows name the same one
- expert_weights: float32 [96, 8], P(('groups', 'ctx')), parts along dimension 0, may hold values from 0.03 to 0.4
Outputs:
- layer_out: bfloat16 [96, 2048], P(('groups', 'ctx')), parts along dimension 0
The draws below stay inside these ranges and needn't reach their ends.
There are 2 independent parts, one for each index of `groups`. The reference program is written for one: setup_inputs(seed, part) draws one part's arguments, and reference() takes and returns one part's arrays. A program takes and returns all parts, laid end to end along the dimension named above; an argument that names none is the same for every part. Nothing has to cross between parts.
Inputs may be any that keep to these rules, and one draw needn't show every extreme that they name: `cache_lengths`: some shard in every draw is full, with 128 live positions. `expert_ids`: within one block of 3 rows no expert is named more than 3 times, a bound that some block reaches.
All inputs are finite; a program needn't handle non-finite values.
Results may differ from the reference program's by a relative error of at most 0.01.
Values may be sent and summed in bfloat16 or wider, within the bound.
No kernel may reach another device: no remote copies, remote signals or barrier semaphores. Data moves between devices by JAX's collectives and lax.ppermute only.
A program may use at most 64 MiB of HBM per device.

```python
import math
import jax
import jax.numpy as jnp
import numpy as np
from jax import lax

D = 2048
HEADS = 32
KV_HEADS = 4
HEAD_DIM = 128
FF = 768
TOP = 8
C_DEV = 128
ROWS_DEV = 3
CAP = 3
SHARDS = 16
EXPERTS = 16
ROWS = 48
CACHE = 2048
WQ = 4096
KVW = 512


def shard_lengths(key):
    first, second = jax.random.split(jax.random.fold_in(key, 11))
    base = jax.random.randint(first, (SHARDS,), 0, C_DEV // 2 + 1)
    chosen = jax.random.randint(second, (), 0, SHARDS)
    lengths = jnp.where(jnp.arange(SHARDS) == chosen, C_DEV, base)
    return lengths.astype(jnp.int32)


def cache_rows(key):
    rows_f = jax.random.truncated_normal(jax.random.fold_in(key, 23), -6.0, 6.0, (CACHE, KV_HEADS, HEAD_DIM), jnp.float32)
    return rows_f


def draw_cache_lengths(key, part):
    return shard_lengths(key)


def draw_cache_keys(key, part):
    return cache_rows(key).reshape(CACHE, KV_HEADS * HEAD_DIM).astype(jnp.bfloat16)


def draw_queries(key, part):
    draws = jax.random.truncated_normal(jax.random.fold_in(key, 37), -6.0, 6.0, (ROWS, HEADS, HEAD_DIM), jnp.float32)
    return draws.reshape(ROWS, HEADS * HEAD_DIM).astype(jnp.bfloat16)


def block_scale(stream_key, extent, shards, low, largest):
    level, own = 1.0, jax.random.fold_in(stream_key, 6)
    for axis_at, parts in shards:
        heights = jnp.exp(jax.random.uniform(jax.random.fold_in(own, axis_at), (parts,), jnp.float32, low / len(shards), largest / len(shards)))
        level = level * jnp.repeat(heights, extent[axis_at] // parts).reshape([-1 if axis == axis_at else 1 for axis in range(len(extent))])
    return level


def assign_block(stream_key, own, number, rows, amount, top, reach, lean):
    sequence = jax.random.permutation(stream_key, amount)
    packed, ordinary = shares(amount, rows * top, reach, lean, True), shares(amount, rows * top, reach, lean, False)
    places = jnp.arange(amount)

    def named(sizes, rotation):
        used = int((sizes > 0).sum())
        fixed = max(1, used // 4)
        moved = fixed + (places - fixed + rotation * (used - fixed)) % max(1, amount - fixed)
        return jnp.zeros((amount,), jnp.int32).at[sequence[jnp.where(places < fixed, places, moved)]].set(jnp.asarray(sizes, jnp.int32))

    sizes = jnp.where(number % 4 == 0, named(packed, number // 4), named(ordinary, number - number // 4 - 1))
    mixed = jax.random.permutation(jax.random.fold_in(own, 3), amount)
    source_of, receiver = mixed[0:amount // 2 * 2:2], mixed[1:amount // 2 * 2:2]
    margin = jnp.minimum(sizes[source_of] - 1, reach - sizes[receiver]) // 2
    margin = jnp.where((source_of == sequence[0]) | (receiver == sequence[0]) | (sizes[receiver] == 0), 0, jnp.maximum(margin, 0))
    moved = jax.random.randint(jax.random.fold_in(own, 4), (amount // 2,), 0, 1 << 20) % (margin + 1)
    sizes = sizes.at[source_of].add(-moved).at[receiver].add(moved)
    items = jnp.searchsorted(jnp.cumsum(sizes), jnp.arange(rows * top), side="right").astype(jnp.int32)
    table = items.reshape(top, rows).T
    table = table[jax.random.permutation(jax.random.fold_in(own, 1), rows)]
    rotation = jax.random.randint(jax.random.fold_in(own, 2), (rows, 1), 0, top)
    return jnp.take_along_axis(table, (jnp.arange(top)[None, :] + rotation) % top, axis=1)


def shares(number_of, total, reach, lean, full):
    weights = [(1 << 20) // math.isqrt(rank ** lean) + 1 for rank in range(1, number_of + 1)]
    largest = reach if full else min(reach, max(-(-total // number_of), total * weights[0] // sum(weights)))
    least = 1 if total - largest >= number_of - 1 else 0
    given, rest = [largest] + [least] * (number_of - 1), total - largest - least * (number_of - 1)
    while rest > 0:
        movable = [i for i in range(1, number_of) if given[i] < largest] or [i for i in range(1, number_of) if given[i] < reach]
        whole, remaining = sum([weights[i] for i in movable]), rest
        for i in movable:
            more = min(reach - given[i], max(1, remaining * weights[i] // whole), rest)
            given[i] = given[i] + more
            rest = rest - more
    return np.array(given)


def bell_draw(own_key, extent, spread, reach, pieces=(), held_as=jnp.bfloat16):
    values = spread * jax.random.normal(own_key, extent, jnp.float32)
    if pieces:
        values = values * block_scale(own_key, extent, pieces, -0.22, 0.18)
    return jnp.clip(values, -reach, reach).astype(held_as)


def setup_inputs(seed: int = 0, part: int = 0) -> dict:
    key_of = jax.random.split(jax.random.key(seed), 15)
    part_splits = jax.random.split(jax.random.fold_in(key_of[14], part), 15)
    queries = draw_queries(jax.random.fold_in(jax.random.fold_in(key_of[14], part), 71), part)
    cache_keys = draw_cache_keys(jax.random.fold_in(jax.random.fold_in(key_of[14], part), 71), part)
    cache_values = bell_draw(part_splits[2], (CACHE, KVW), 1.0, 6.0, ((0, 16),))
    new_keys = bell_draw(part_splits[3], (ROWS, KVW), 1.0, 6.0, ((0, 16),))
    new_values = bell_draw(part_splits[4], (ROWS, KVW), 1.0, 6.0, ((0, 16),))
    cache_lengths = draw_cache_lengths(jax.random.fold_in(jax.random.fold_in(key_of[14], part), 71), part)
    residual_in = bell_draw(part_splits[6], (ROWS, D), 1.0, 6.0, ((0, 16),))
    out_weight = bell_draw(key_of[7], (WQ, D), 0.5, 3.0, ((0, 16),))
    norm_gain = jnp.clip(1.0 + 0.15 * jax.random.normal(key_of[8], (D,), jnp.float32), 0.25, 1.75).astype(jnp.bfloat16)
    expert_gate = bell_draw(key_of[9], (EXPERTS, D, FF), D ** -0.5, 0.125, ((0, 16),))
    expert_up = bell_draw(key_of[10], (EXPERTS, D, FF), D ** -0.5, 0.125, ((0, 16),))
    expert_down = bell_draw(key_of[11], (EXPERTS, FF, D), FF ** -0.5, 0.21875, ((0, 16),))
    expert_ids_keys = jax.random.split(jax.random.fold_in(part_splits[12], 1), ROWS // ROWS_DEV)
    expert_ids_turns = jax.random.permutation(jax.random.fold_in(part_splits[12], 3), ROWS // ROWS_DEV)
    expert_ids = jax.vmap(lambda own, number: assign_block(jax.random.fold_in(part_splits[12], 2), own, number, ROWS_DEV, EXPERTS, TOP, CAP, 2))(expert_ids_keys, expert_ids_turns).reshape((ROWS, TOP))
    expert_weights = jnp.clip(jnp.exp(math.log(0.4) - 2.5902672 * jax.random.uniform(part_splits[13], (ROWS, TOP), jnp.float32) ** block_scale(part_splits[13], (ROWS, TOP), ((0, 16),), -0.2, 0.2)), 0.03, 0.4)
    return {"queries": queries, "cache_keys": cache_keys, "cache_values": cache_values, "new_keys": new_keys, "new_values": new_values, "cache_lengths": cache_lengths, "residual_in": residual_in, "out_weight": out_weight, "norm_gain": norm_gain, "expert_gate": expert_gate, "expert_up": expert_up, "expert_down": expert_down, "expert_ids": expert_ids, "expert_weights": expert_weights}


MASKED = -1e+30
epsilon = 1e-06

def slot_numbers(block_ids):
    flat_ids = block_ids.reshape(-1)
    count = flat_ids.shape[0]
    places = jnp.arange(count, dtype=jnp.int32)
    earlier = (flat_ids[:, None] == flat_ids[None, :]) & (places[None, :] < places[:, None])
    ranks = lax.optimization_barrier(jnp.sum(earlier.astype(jnp.int32), axis=1))
    return (flat_ids * CAP + ranks).astype(jnp.int32)

def reference(queries, cache_keys, cache_values, new_keys, new_values, cache_lengths, residual_in, out_weight, norm_gain, expert_gate, expert_up, expert_down, expert_ids, expert_weights):
    group_size = HEADS // KV_HEADS
    query_heads = queries.reshape(ROWS, HEADS, HEAD_DIM)
    key_rows = jnp.concatenate([cache_keys, new_keys], 0).reshape(CACHE + ROWS, KV_HEADS, HEAD_DIM)
    value_rows = jnp.concatenate([cache_values, new_values], 0).reshape(CACHE + ROWS, KV_HEADS, HEAD_DIM)
    positions = jnp.arange(CACHE, dtype=jnp.int32)
    cache_ok = positions % C_DEV < cache_lengths[positions // C_DEV]
    row_ids = jnp.arange(ROWS, dtype=jnp.int32)
    span_ok = row_ids[None, :] <= row_ids[:, None]
    usable = jnp.concatenate([jnp.broadcast_to(cache_ok[None, :], (ROWS, CACHE)), span_ok], 1)

    def single_head(head):
        query_one = lax.dynamic_index_in_dim(query_heads, head, 1, False)
        key_one = lax.dynamic_index_in_dim(key_rows, head // group_size, 1, False)
        value_one = lax.dynamic_index_in_dim(value_rows, head // group_size, 1, False)
        scores = jnp.dot(query_one, key_one.T, preferred_element_type=jnp.float32) * HEAD_DIM ** (-0.5)
        scores = jnp.where(usable, scores, MASKED)
        maxima = lax.optimization_barrier(jnp.max(scores, axis=1, keepdims=True))
        exp_weights = jnp.where(usable, jnp.exp(scores - maxima), 0.0)
        totals = lax.optimization_barrier(jnp.sum(exp_weights, axis=1, keepdims=True))
        summed = jnp.dot(exp_weights.astype(jnp.bfloat16), value_one, preferred_element_type=jnp.float32)
        return summed / totals
    heads_out = lax.map(single_head, jnp.arange(HEADS, dtype=jnp.int32))
    attention = heads_out.transpose(1, 0, 2).reshape(ROWS, WQ).astype(jnp.bfloat16)
    projected = jnp.dot(attention, out_weight, preferred_element_type=jnp.float32)
    state = residual_in.astype(jnp.float32) + projected
    normed = (state * lax.rsqrt(lax.optimization_barrier(jnp.mean(state * state, axis=1, keepdims=True)) + epsilon) * norm_gain.astype(jnp.float32)).astype(jnp.bfloat16)
    n_slots = EXPERTS * CAP
    slot_of = jax.vmap(slot_numbers)(expert_ids.reshape(SHARDS, ROWS_DEV, TOP))
    one_hot = (slot_of[:, :, None] == jnp.arange(n_slots, dtype=jnp.int32)[None, None, :]).astype(jnp.float32)
    dispatch_map = one_hot.reshape(SHARDS, ROWS_DEV, TOP, n_slots).sum(2)
    normed_blocks = normed.reshape(SHARDS, ROWS_DEV, D).astype(jnp.float32)
    outgoing = jnp.einsum('srn,srd->snd', dispatch_map, normed_blocks, precision=lax.Precision.HIGHEST).astype(jnp.bfloat16)
    outgoing = outgoing.reshape(SHARDS, EXPERTS, CAP, D).transpose(1, 0, 2, 3)

    def expert_work(inputs):
        received, gate_w, up_w, down_w = inputs
        flat_rows = received.reshape(SHARDS * CAP, D)
        gate_out = jnp.dot(flat_rows, gate_w, preferred_element_type=jnp.float32)
        up_out = jnp.dot(flat_rows, up_w, preferred_element_type=jnp.float32)
        activated = (jax.nn.silu(gate_out) * up_out).astype(jnp.bfloat16)
        expert_out = jnp.dot(activated, down_w, preferred_element_type=jnp.float32).astype(jnp.bfloat16)
        return expert_out.reshape(SHARDS, CAP, D)
    results = lax.map(expert_work, (outgoing, expert_gate, expert_up, expert_down))
    back = results.transpose(1, 0, 2, 3).reshape(SHARDS, n_slots, D)
    combine_map = (one_hot * expert_weights.reshape(SHARDS, ROWS_DEV * TOP)[:, :, None]).reshape(SHARDS, ROWS_DEV, TOP, n_slots).sum(2)
    expert_sum = jnp.einsum('srn,snd->srd', combine_map, back.astype(jnp.float32), precision=lax.Precision.HIGHEST).reshape(ROWS, D)
    return (state + expert_sum).astype(jnp.bfloat16)
```

```python
import jax
import jax.numpy as jnp
from jax import lax
from jax.sharding import PartitionSpec as P

HEADS = 32
KV_HEADS = 4
HEAD_DIM = 128
TOP = 8


MASKED = -1e30
epsilon = 1e-06


def spread(block, shards):
    copies = jnp.broadcast_to(block[None], (shards,) + block.shape)
    return lax.all_to_all(copies, "ctx", split_axis=0, concat_axis=0, tiled=True)


def local(
    queries,
    cache_keys,
    cache_values,
    new_keys,
    new_values,
    cache_lengths,
    residual_in,
    out_weight,
    norm_gain,
    expert_gate,
    expert_up,
    expert_down,
    expert_ids,
    expert_weights,
):
    shards = lax.axis_size("ctx")
    device = lax.axis_index("ctx")
    rows_dev, width = residual_in.shape
    all_rows = rows_dev * shards
    group_size = HEADS // KV_HEADS
    columns_dev = out_weight.shape[0]
    whole_queries = spread(queries, shards).reshape(all_rows, HEADS * HEAD_DIM)
    query_heads = whole_queries.reshape(all_rows, KV_HEADS, group_size, HEAD_DIM)
    local_cache = cache_keys.shape[0]
    key_rows = jnp.concatenate([cache_keys, new_keys], 0).reshape(
        local_cache + rows_dev, KV_HEADS, HEAD_DIM
    )
    value_rows = jnp.concatenate([cache_values, new_values], 0).reshape(
        local_cache + rows_dev, KV_HEADS, HEAD_DIM
    )
    slot_ids = jnp.arange(local_cache + rows_dev, dtype=jnp.int32)
    span_pos = device * rows_dev + slot_ids - local_cache
    row_ids = jnp.arange(all_rows, dtype=jnp.int32)
    usable = jnp.where(
        slot_ids[None, :] < local_cache,
        (slot_ids < cache_lengths[0])[None, :],
        span_pos[None, :] <= row_ids[:, None],
    )
    scores = jnp.einsum(
        "rkgd,nkd->kgrn", query_heads, key_rows, preferred_element_type=jnp.float32
    ) * HEAD_DIM ** (-0.5)
    scores = jnp.where(usable, scores, MASKED)
    maxima = jnp.max(scores, axis=-1).astype(jnp.bfloat16)
    exp_weights = jnp.where(
        usable, jnp.exp(scores - maxima.astype(jnp.float32)[..., None]), 0.0
    )
    totals = jnp.sum(exp_weights, axis=-1)
    numerators = jnp.einsum(
        "kgrn,nkd->rkgd",
        exp_weights.astype(jnp.bfloat16),
        value_rows,
        preferred_element_type=jnp.float32,
    ).reshape(all_rows, HEADS * HEAD_DIM)
    maxima = maxima.transpose(2, 0, 1).reshape(all_rows, HEADS)
    totals = totals.transpose(2, 0, 1).reshape(all_rows, HEADS)
    totals_high = totals.astype(jnp.bfloat16)
    totals_low = (totals - totals_high.astype(jnp.float32)).astype(jnp.bfloat16)
    heads_dev = max(1, columns_dev // HEAD_DIM)
    repeats = shards * heads_dev // HEADS
    stats = jnp.stack([maxima, totals_high, totals_low], 0)
    stats = jnp.repeat(stats, repeats, axis=2).reshape(3, all_rows, shards, heads_dev)
    stats = stats.transpose(2, 0, 3, 1).reshape(shards, 3 * heads_dev, all_rows)
    pieces = (
        numerators.astype(jnp.bfloat16)
        .reshape(all_rows, shards, columns_dev)
        .transpose(1, 0, 2)
    )
    lanes = -(-all_rows // columns_dev)
    stats = jnp.pad(stats, ((0, 0), (0, 0), (0, lanes * columns_dev - all_rows)))
    stats = stats.reshape(shards, 3 * heads_dev * lanes, columns_dev)
    got = lax.all_to_all(
        jnp.concatenate([pieces, stats], 1), "ctx", split_axis=0, concat_axis=0, tiled=True
    )
    parts = got[:, :all_rows].astype(jnp.float32)
    stats = got[:, all_rows:].reshape(shards, 3, heads_dev, lanes * columns_dev)[..., :all_rows]
    stats = stats.astype(jnp.float32)
    maxima, totals = stats[:, 0], stats[:, 1] + stats[:, 2]
    largest = jnp.max(maxima, axis=0)
    rescale = jnp.exp(maxima - largest)
    scale = rescale / jnp.sum(totals * rescale, axis=0)
    scale = jnp.repeat(scale.transpose(0, 2, 1), columns_dev // heads_dev, axis=2)
    columns = jnp.sum(parts * scale, axis=0).astype(jnp.bfloat16)
    projected = jnp.dot(columns, out_weight, preferred_element_type=jnp.float32)
    received = lax.all_to_all(
        projected.astype(jnp.bfloat16).reshape(shards, rows_dev, width),
        "ctx",
        split_axis=0,
        concat_axis=0,
        tiled=True,
    )
    projected = jnp.sum(received.astype(jnp.float32), axis=0)
    state = residual_in.astype(jnp.float32) + projected
    normed = (
        state
        * lax.rsqrt(jnp.mean(state * state, axis=1, keepdims=True) + epsilon)
        * norm_gain.astype(jnp.float32)
    ).astype(jnp.bfloat16)
    every = spread(normed, shards).reshape(all_rows, width)
    gate_out = jnp.dot(every, expert_gate[0], preferred_element_type=jnp.float32)
    up_out = jnp.dot(every, expert_up[0], preferred_element_type=jnp.float32)
    activated = (jax.nn.silu(gate_out) * up_out).astype(jnp.bfloat16)
    expert_out = jnp.dot(
        activated, expert_down[0], preferred_element_type=jnp.float32
    ).astype(jnp.bfloat16)
    back = lax.all_to_all(
        expert_out.reshape(shards, rows_dev, width), "ctx", split_axis=0, concat_axis=0, tiled=True
    )
    experts = jnp.arange(shards, dtype=jnp.int32)
    chosen = jnp.sum(
        jnp.where(
            expert_ids[:, :, None] == experts[None, None, :], expert_weights[:, :, None], 0.0
        ),
        axis=1,
    )
    expert_sum = jnp.sum(back.astype(jnp.float32) * chosen.T[:, :, None], axis=0)
    return (state + expert_sum).astype(jnp.bfloat16)


def solution(mesh):
    placed = (
        P(("groups", "ctx"), None),
        P(("groups", "ctx"), None),
        P(("groups", "ctx"), None),
        P(("groups", "ctx"), None),
        P(("groups", "ctx"), None),
        P(("groups", "ctx")),
        P(("groups", "ctx"), None),
        P("ctx", None),
        P(),
        P("ctx", None, None),
        P("ctx", None, None),
        P("ctx", None, None),
        P(("groups", "ctx"), None),
        P(("groups", "ctx"), None),
    )
    return jax.shard_map(
        local, mesh=mesh, in_specs=placed, out_specs=P(("groups", "ctx"), None), check_vma=False
    )
```

```python
import functools

import jax
import jax.numpy as jnp
from jax import lax
from jax.experimental import pallas as pl
from jax.experimental.pallas import tpu as pltpu
from jax.sharding import PartitionSpec as P

HEADS = 32
KV_HEADS = 4
HEAD_DIM = 128
GROUP = HEADS // KV_HEADS

MASKED = -1e30
epsilon = 1e-06

f32, bf16 = jnp.float32, jnp.bfloat16
VMEM = pl.BlockSpec(memory_space=pltpu.VMEM)
SMEM = pl.BlockSpec(memory_space=pltpu.SMEM)


def coordinates(inner):
    device = lax.axis_index("ctx")
    return device // inner, lax.rem(device, inner)


def call(body, outs, scratch=(), grant=4, **settings):
    return pl.pallas_call(
        body,
        out_shape=outs,
        out_specs=jax.tree.map(lambda _: VMEM, outs),
        scratch_shapes=list(scratch),
        compiler_params=pltpu.CompilerParams(vmem_limit_bytes=grant << 20),
        cost_estimate=pl.CostEstimate(
            flops=10**9, bytes_accessed=10**6, transcendentals=0
        ),
        **settings,
    )


def pack(outer, inner, rows, cache, *refs):
    (lengths, keys, values, new_keys, new_values), refs = refs[:5], refs[5:]
    queries, refs = refs[:inner], refs[inner:]
    outs, (small, wide) = refs[:outer], refs[outer:]
    a, _ = coordinates(inner)
    length = lengths[0].astype(f32)
    per_row = rows * GROUP
    for k in range(outer):
        head = jnp.bitwise_xor(a, k)
        lanes = pl.ds(pl.multiple_of(head * HEAD_DIM, HEAD_DIM), HEAD_DIM)
        base = 0
        for old, new in ((keys, new_keys), (values, new_values)):
            outs[k][base : base + cache] = old[:, lanes]
            small[...] = jnp.zeros_like(small)
            small[0:rows] = new[:, lanes].astype(f32)
            small[rows : rows + 1] = jnp.full((1, HEAD_DIM), length, f32)
            outs[k][base + cache : base + cache + 16] = small[...].astype(bf16)
            base += cache + 16
        lanes = pl.ds(
            pl.multiple_of(head * GROUP * HEAD_DIM, GROUP * HEAD_DIM), GROUP * HEAD_DIM
        )
        for m in range(inner):
            block = queries[m][:, lanes].astype(f32)
            for g in range(GROUP):
                at = m * per_row + g * rows
                wide[at : at + rows] = block[:, g * HEAD_DIM : (g + 1) * HEAD_DIM]
        outs[k][base:] = wide[...].astype(bf16)


def places(outer, inner, rows, padded):
    i = lax.broadcasted_iota(jnp.int32, (inner * padded, 1), 0)
    b = i // padded if padded & (padded - 1) else jnp.right_shift(i, padded.bit_length() - 1)
    rest = i - b * padded
    a = jnp.right_shift(rest * (-(-65536 // rows)), 16)
    return a, b, rest - a * rows, rest < outer * rows


def attend(outer, inner, rows, cache, padded, heads, step, *refs):
    blocks, refs = refs[:outer], refs[outer:]
    outs, (asked, parts) = refs[:inner], refs[inner:]
    a, b = coordinates(inner)
    per_row = rows * GROUP
    count = inner * padded
    length = cache + 16
    at_a, at_b, at_r, valid = places(outer, inner, rows, padded)
    gathered = jnp.concatenate([block[2 * length :] for block in blocks], 0)
    source = jnp.bitwise_xor(at_a, a) * (inner * per_row) + jnp.bitwise_xor(at_b, b) * per_row + at_r
    source = jnp.where(valid, source, -GROUP * rows)
    column = lax.broadcasted_iota(jnp.int32, (count, gathered.shape[0]), 1)
    for g in range(GROUP):
        pick = jnp.where(column == source + g * rows, 1.0, 0.0).astype(bf16)
        asked[g * count : (g + 1) * count] = jnp.dot(
            pick, gathered, preferred_element_type=f32
        ).astype(bf16)
    position = rows * (at_a * inner + at_b) + at_r
    slot = lax.broadcasted_iota(jnp.int32, (count, length), 1)
    wanted = asked[...]
    scores, usable = [], []
    for k in range(outer):
        live = blocks[k][cache : cache + 16].astype(f32)[rows : rows + 1, 0:1]
        span = rows * (jnp.bitwise_xor(a, k) * inner + b) + slot - cache
        room = jnp.where(
            slot < cache,
            live - slot.astype(f32),
            jnp.where(slot < cache + rows, position - span + 1, 0).astype(f32),
        )
        ok = room > 0.0
        usable.append(ok[None])
        s = lax.dot_general(
            wanted, blocks[k][0:length], (((1,), (1,)), ((), ())), preferred_element_type=f32
        ) * HEAD_DIM ** (-0.5)
        scores.append(jnp.where(ok[None], s.reshape(GROUP, count, length), MASKED))
    largest = functools.reduce(
        jnp.maximum, [jnp.max(s, axis=-1, keepdims=True) for s in scores]
    )
    largest = largest.astype(bf16).astype(f32)
    total = jnp.zeros((GROUP, count, 1), f32)
    summed = jnp.zeros((GROUP * count, HEAD_DIM), f32)
    for k in range(outer):
        e = jnp.where(usable[k], jnp.exp(scores[k] - largest), 0.0)
        total = total + jnp.sum(e, axis=-1, keepdims=True)
        summed = summed + jnp.dot(
            e.reshape(GROUP * count, length).astype(bf16),
            blocks[k][length : 2 * length],
            preferred_element_type=f32,
        )
    total = total.reshape(GROUP * count, 1)
    high = total.astype(bf16).astype(f32)
    lane = lax.broadcasted_iota(jnp.int32, (GROUP * count, HEAD_DIM), 1)
    stats = jnp.where(
        lane == 0,
        largest.reshape(GROUP * count, 1),
        jnp.where(lane == 1, high, total - high),
    )
    parts[:, 0:HEAD_DIM] = summed.astype(bf16)
    parts[:, HEAD_DIM:] = stats.astype(bf16)
    for k in range(inner):
        first = jnp.right_shift(jnp.bitwise_xor(b, k) * step, HEAD_DIM.bit_length() - 1)
        outs[k][...] = parts[pl.ds(pl.multiple_of(first * count, 16), heads * count)]


def project(inner, padded, heads, *refs):
    chunks, refs = refs[:inner], refs[inner:]
    weight, own, outs, total = refs[0], refs[1], refs[2 : inner + 1], refs[inner + 1]
    _, b = coordinates(inner)
    count = inner * padded
    stats = [chunk[:, HEAD_DIM:].astype(f32) for chunk in chunks]
    largest = functools.reduce(jnp.maximum, [s[:, 0:1] for s in stats])
    scales = [jnp.exp(s[:, 0:1] - largest) for s in stats]
    denominator = sum(w * (s[:, 1:2] + s[:, 2:3]) for w, s in zip(scales, stats))
    joined = sum(
        chunk[:, 0:HEAD_DIM].astype(f32) * (w / denominator)
        for w, chunk in zip(scales, chunks)
    ).astype(bf16)
    total[...] = sum(
        jnp.dot(
            joined[h * count : (h + 1) * count],
            weight[h * HEAD_DIM : (h + 1) * HEAD_DIM],
            preferred_element_type=f32,
        )
        for h in range(heads)
    )
    own[...] = total[pl.ds(pl.multiple_of(b * padded, padded), padded)]
    for k in range(1, inner):
        at = pl.multiple_of(jnp.bitwise_xor(b, k) * padded, padded)
        outs[k - 1][...] = total[pl.ds(at, padded)].astype(bf16)


def add_up(inner, rows, own, residual, *refs):
    others, (kept, sent) = refs[:-2], refs[-2:]
    a, _ = coordinates(inner)
    partial = own[...]
    for other in others:
        partial = partial + other[...].astype(f32)
    row = lax.broadcasted_iota(jnp.int32, partial.shape, 0)
    start = residual[...].astype(f32)
    for r in range(rows):
        partial = partial + jnp.where(row == a * rows + r, start[r : r + 1], 0.0)
    kept[...] = partial
    sent[...] = partial.astype(bf16)


def normalise(inner, rows, kept, gain, *refs):
    others, (normed, mine) = refs[:-2], refs[-2:]
    a, _ = coordinates(inner)
    state = kept[...]
    for other in others:
        state = state + other[...].astype(f32)
    mean = jnp.mean(state * state, axis=1, keepdims=True)
    normed[...] = (state * lax.rsqrt(mean + epsilon) * gain[...].astype(f32)).astype(bf16)
    row = lax.broadcasted_iota(jnp.int32, state.shape, 0)
    for r in range(rows):
        mine[r : r + 1] = jnp.sum(
            jnp.where(row == a * rows + r, state, 0.0), axis=0, keepdims=True
        )


def expert(outer, inner, rows, padded, gate, up, down, *refs):
    classes, (out, held) = refs[:inner], refs[inner:]
    _, b = coordinates(inner)
    x = jnp.concatenate([c[...] for c in classes], 0)
    gated = jnp.dot(x, gate[0], preferred_element_type=f32)
    lifted = jnp.dot(x, up[0], preferred_element_type=f32)
    active = (gated / (1.0 + jnp.exp(-gated)) * lifted).astype(bf16)
    held[...] = jnp.dot(active, down[0], preferred_element_type=f32)
    for k in range(inner):
        for s in range(outer):
            at = k * padded + s * rows
            out[s * inner + jnp.bitwise_xor(b, k)] = held[at : at + rows].astype(bf16)


def combine(state, back, ids, weights, out):
    total = state[...]
    chosen, weight = ids[...], weights[...]
    for e in range(back.shape[0]):
        share = jnp.sum(jnp.where(chosen == e, weight, 0.0), axis=1, keepdims=True)
        total = total + share * back[e].astype(f32)
    out[...] = total.astype(bf16)


def local(
    queries,
    cache_keys,
    cache_values,
    new_keys,
    new_values,
    cache_lengths,
    residual_in,
    out_weight,
    norm_gain,
    expert_gate,
    expert_up,
    expert_down,
    expert_ids,
    expert_weights,
):
    shards = lax.axis_size("ctx")
    outer = KV_HEADS
    inner = shards // outer
    rows, width = residual_in.shape
    cache = cache_keys.shape[0]
    padded = max(16, 1 << (outer * rows - 1).bit_length())
    count = inner * padded
    step = out_weight.shape[0]
    heads = max(1, step // HEAD_DIM)

    def outward(x, k):
        pairs = [(i, ((i // inner) ^ k) * inner + i % inner) for i in range(shards)]
        return lax.ppermute(x, "ctx", pairs)

    def inward(x, k):
        pairs = [(i, i // inner * inner + ((i % inner) ^ k)) for i in range(shards)]
        return lax.ppermute(x, "ctx", pairs)

    asked = [queries] + [inward(queries, k) for k in range(1, inner)]
    asked_rows = inner * rows * GROUP
    block = jax.ShapeDtypeStruct((2 * (cache + 16) + asked_rows, HEAD_DIM), bf16)
    blocks = call(
        functools.partial(pack, outer, inner, rows, cache),
        [block] * outer,
        [pltpu.VMEM((16, HEAD_DIM), f32), pltpu.VMEM((asked_rows, HEAD_DIM), f32)],
        in_specs=[SMEM] + [VMEM] * (4 + inner),
    )(cache_lengths, cache_keys, cache_values, new_keys, new_values, *asked)
    blocks = [blocks[0]] + [outward(blocks[k], k) for k in range(1, outer)]

    chunk = jax.ShapeDtypeStruct((heads * count, 2 * HEAD_DIM), bf16)
    chunks = call(
        functools.partial(attend, outer, inner, rows, cache, padded, heads, step),
        [chunk] * inner,
        [
            pltpu.VMEM((GROUP * count, HEAD_DIM), bf16),
            pltpu.VMEM((GROUP * count, 2 * HEAD_DIM), bf16),
        ],
        grant=max(8, count // 8),
        in_specs=[VMEM] * outer,
    )(*blocks)
    chunks = [chunks[0]] + [inward(chunks[k], k) for k in range(1, inner)]

    if step < HEAD_DIM:
        at = lax.rem(lax.axis_index("ctx") * step, HEAD_DIM)
        out_weight = lax.dynamic_update_slice(
            jnp.zeros((HEAD_DIM, width), out_weight.dtype), out_weight, (at, 0)
        )
    part = jax.ShapeDtypeStruct((padded, width), bf16)
    whole = jax.ShapeDtypeStruct((padded, width), f32)
    own, *parts = call(
        functools.partial(project, inner, padded, heads),
        [whole] + [part] * (inner - 1),
        [pltpu.VMEM((count, width), f32)],
        grant=max(4, count // 16),
        in_specs=[VMEM] * (inner + 1),
    )(*chunks, out_weight)
    parts = [inward(parts[k - 1], k) for k in range(1, inner)]

    kept, sent = call(
        functools.partial(add_up, inner, rows), [whole, part], in_specs=[VMEM] * (inner + 1)
    )(own, residual_in, *parts)
    others = [outward(sent, k) for k in range(1, outer)]
    normed, state = call(
        functools.partial(normalise, inner, rows),
        [part, jax.ShapeDtypeStruct((rows, width), f32)],
        in_specs=[VMEM] * (outer + 1),
    )(kept, norm_gain.reshape(1, width), *others)
    classes = [normed] + [inward(normed, k) for k in range(1, inner)]

    results = call(
        functools.partial(expert, outer, inner, rows, padded),
        jax.ShapeDtypeStruct((shards, rows, width), bf16),
        [pltpu.VMEM((count, width), f32)],
        grant=max(8, count // 8),
        in_specs=[VMEM] * (inner + 3),
    )(expert_gate, expert_up, expert_down, *classes)
    back = lax.all_to_all(results, "ctx", split_axis=0, concat_axis=0, tiled=True)
    return call(
        combine, jax.ShapeDtypeStruct((rows, width), bf16), in_specs=[VMEM] * 4
    )(state, back, expert_ids, expert_weights)


def solution(mesh):
    placed = (
        P(("groups", "ctx"), None),
        P(("groups", "ctx"), None),
        P(("groups", "ctx"), None),
        P(("groups", "ctx"), None),
        P(("groups", "ctx"), None),
        P(("groups", "ctx")),
        P(("groups", "ctx"), None),
        P("ctx", None),
        P(),
        P("ctx", None, None),
        P("ctx", None, None),
        P("ctx", None, None),
        P(("groups", "ctx"), None),
        P(("groups", "ctx"), None),
    )
    return jax.shard_map(
        local, mesh=mesh, in_specs=placed, out_specs=P(("groups", "ctx"), None), check_vma=False
    )
```

```python
import functools

import jax
import jax.numpy as jnp
from jax import lax
from jax.experimental import pallas as pl
from jax.experimental.pallas import tpu as pltpu
from jax.sharding import PartitionSpec as P

HEADS = 32
KV_HEADS = 4
HEAD_DIM = 128
GROUP = HEADS // KV_HEADS
LANES = 128

MASKED = -1e30
epsilon = 1e-06

f32, bf16 = jnp.float32, jnp.bfloat16
VMEM = pl.BlockSpec(memory_space=pltpu.VMEM)


def coordinates(inner):
    device = lax.axis_index("ctx")
    return device // inner, lax.rem(device, inner)


def call(body, outs, operands, scratch=(), grant=4, flops=10**9):
    return pl.pallas_call(
        body,
        out_shape=outs,
        in_specs=[VMEM] * len(operands),
        out_specs=jax.tree.map(lambda _: VMEM, outs),
        scratch_shapes=list(scratch),
        compiler_params=pltpu.CompilerParams(vmem_limit_bytes=grant << 20),
        cost_estimate=pl.CostEstimate(flops=flops, bytes_accessed=10**6, transcendentals=0),
    )(*operands)


def aligned(index, size):
    return pl.ds(pl.multiple_of(index * size, size), size)


def pack_span(outer, inner, rows, token, lengths, new_keys, new_values, queries, *refs):
    outs, wide = refs[:outer], refs[outer]
    a, _ = coordinates(inner)
    per_row = rows * GROUP
    live = lengths[...].astype(f32).reshape(1, 1)
    wide[...] = jnp.zeros_like(wide)
    wide[per_row + 2 * rows : per_row + 2 * rows + 1] = jnp.broadcast_to(live, (1, HEAD_DIM))
    for k in range(outer):
        head = jnp.bitwise_xor(a, k)
        lanes = aligned(head, HEAD_DIM)
        block = queries[:, aligned(head, GROUP * HEAD_DIM)].astype(f32)
        for g in range(GROUP):
            wide[g * rows : (g + 1) * rows] = block[:, g * HEAD_DIM : (g + 1) * HEAD_DIM]
        wide[per_row : per_row + rows] = new_keys[:, lanes].astype(f32)
        wide[per_row + rows : per_row + 2 * rows] = new_values[:, lanes].astype(f32)
        outs[k][...] = wide[...].astype(bf16)


def pack_cache(outer, inner, keys, values, *outs):
    a, _ = coordinates(inner)
    cache = keys.shape[0]
    for k in range(outer):
        lanes = aligned(jnp.bitwise_xor(a, k), HEAD_DIM)
        outs[k][0:cache] = keys[:, lanes]
        outs[k][cache:] = values[:, lanes]


def plan(outer, inner, rows, count, pick, token):
    a, b = coordinates(inner)
    per_row = rows * GROUP
    position = lax.broadcasted_iota(jnp.int32, (count, 1), 0)
    owner = jnp.right_shift(position * (-(-65536 // rows)), 16)
    at_a = jnp.bitwise_xor(jnp.right_shift(owner, inner.bit_length() - 1), a)
    at_b = jnp.bitwise_xor(jnp.bitwise_and(owner, inner - 1), b)
    source = (at_b * outer + at_a) * per_row + position - owner * rows
    source = jnp.where(owner < outer * inner, source, -per_row)
    column = lax.broadcasted_iota(jnp.int32, (count, pick.shape[1]), 1)
    for g in range(GROUP):
        pick[g * count : (g + 1) * count] = jnp.where(
            column == source + g * rows, 1.0, 0.0
        ).astype(bf16)
    token[...] = jnp.zeros_like(token)


def collect(outer, rows, *refs):
    spans, out, wide = refs[:outer], refs[outer], refs[outer + 1]
    per_row = rows * GROUP
    for k in range(outer):
        wide[k * per_row : (k + 1) * per_row] = spans[k][...].astype(f32)[0:per_row]
    out[...] = wide[...].astype(bf16)


def attend(outer, inner, rows, count, heads, step, *refs):
    pick, spans, caches = refs[0], refs[1 : outer + 1], refs[outer + 1 : 2 * outer + 1]
    queries, refs = refs[2 * outer + 1 : 2 * outer + 1 + inner], refs[2 * outer + 1 + inner :]
    outs, (fresh, parts) = refs[:inner], refs[inner:]
    a, b = coordinates(inner)
    cache = caches[0].shape[0] // 2
    lines, per_row = spans[0].shape[0], rows * GROUP
    gathered = jnp.concatenate([block[...] for block in queries], 0)
    wanted = jnp.dot(pick[...], gathered, preferred_element_type=f32).astype(bf16)

    def score(keys, usable):
        s = lax.dot_general(
            wanted, keys, (((1,), (1,)), ((), ())), preferred_element_type=f32
        ) * HEAD_DIM ** (-0.5)
        return jnp.where(usable, s.reshape((GROUP, count, keys.shape[0])), MASKED)

    fresh[...] = jnp.zeros_like(fresh)
    position = lax.broadcasted_iota(jnp.int32, (count, outer * lines), 0)
    slot = lax.broadcasted_iota(jnp.int32, (count, outer * lines), 1)
    reach = jnp.full((count, outer * lines), -1, jnp.int32)
    lives = []
    for k in range(outer):
        block = spans[k][...].astype(f32)
        lives.append(block[per_row + 2 * rows : per_row + 2 * rows + 1, 0:1])
        first = k * lines + per_row
        fresh[first : first + rows] = block[per_row + rows : per_row + 2 * rows]
        start = rows * (jnp.bitwise_xor(a, k) * inner + b)
        inside = (slot >= first) & (slot < first + rows)
        reach = jnp.where(inside, position - start - (slot - first), reach)
    keys = [jnp.concatenate([block[...] for block in spans], 0)]
    values = [fresh[...].astype(bf16)]
    usable = [(reach >= 0)[None]]
    index = lax.broadcasted_iota(jnp.int32, (count, cache), 1).astype(f32)
    for k in range(outer):
        keys.append(caches[k][0:cache])
        values.append(caches[k][cache:])
        usable.append(((lives[k] - index) > 0.0)[None])
    scores = [score(key, ok) for key, ok in zip(keys, usable)]
    largest = functools.reduce(
        jnp.maximum, [jnp.max(s, axis=-1, keepdims=True) for s in scores]
    )
    largest = largest.astype(bf16).astype(f32)
    total = jnp.zeros((GROUP, count, 1), f32)
    summed = jnp.zeros((GROUP * count, HEAD_DIM), f32)
    for s, ok, value in zip(scores, usable, values):
        e = jnp.where(ok, jnp.exp(s - largest), 0.0)
        total = total + jnp.sum(e, axis=-1, keepdims=True)
        summed = summed + jnp.dot(
            e.reshape(GROUP * count, value.shape[0]).astype(bf16),
            value,
            preferred_element_type=f32,
        )
    total = total.reshape(GROUP * count, 1)
    high = total.astype(bf16).astype(f32)
    lane = lax.broadcasted_iota(jnp.int32, (GROUP * count, HEAD_DIM), 1)
    stats = jnp.where(
        lane == 0,
        largest.reshape(GROUP * count, 1),
        jnp.where(lane == 1, high, total - high),
    )
    parts[:, 0:HEAD_DIM] = summed.astype(bf16)
    parts[:, HEAD_DIM:] = stats.astype(bf16)
    for k in range(inner):
        first = jnp.right_shift(jnp.bitwise_xor(b, k) * step, HEAD_DIM.bit_length() - 1)
        outs[k][...] = parts[pl.ds(pl.multiple_of(first * count, 16), heads * count)]


def project(inner, rows, count, heads, *refs):
    chunks, (weight, residual), refs = refs[:inner], refs[inner : inner + 2], refs[inner + 2 :]
    own, outs, total = refs[0], refs[1:inner], refs[inner]
    _, b = coordinates(inner)
    stats = [chunk[:, HEAD_DIM:].astype(f32) for chunk in chunks]
    largest = functools.reduce(jnp.maximum, [s[:, 0:1] for s in stats])
    scales = [jnp.exp(s[:, 0:1] - largest) for s in stats]
    denominator = sum(w * (s[:, 1:2] + s[:, 2:3]) for w, s in zip(scales, stats))
    joined = sum(
        chunk[:, 0:HEAD_DIM].astype(f32) * (w / denominator)
        for w, chunk in zip(scales, chunks)
    ).astype(bf16)
    total[...] = sum(
        jnp.dot(
            joined[h * count : (h + 1) * count],
            weight[h * HEAD_DIM : (h + 1) * HEAD_DIM],
            preferred_element_type=f32,
        )
        for h in range(heads)
    )
    start = lax.axis_index("ctx") * rows
    added = residual[...].astype(f32)
    for r in range(rows):
        row = pl.ds(start + r, 1)
        total[row] = total[row] + added[r : r + 1]
    columns = own.shape[1]
    own[...] = total[:, aligned(b, columns)]
    for k in range(1, inner):
        outs[k - 1][...] = total[:, aligned(jnp.bitwise_xor(b, k), columns)].astype(bf16)


def add_up(own, *refs):
    others, (kept, sent) = refs[:-2], refs[-2:]
    partial = own[...]
    for other in others:
        partial = partial + other[...].astype(f32)
    kept[...] = partial
    sent[...] = partial.astype(bf16)


def expert(inner, rows, shards, gate, up, down, gain, *refs):
    pieces, (out, mine, state, normed, held, dense) = refs[:inner], refs[inner:]
    _, b = coordinates(inner)
    columns = pieces[0].shape[1]
    values = [piece[...].astype(f32) for piece in pieces]
    squares = sum(jnp.sum(v * v, axis=1, keepdims=True) for v in values)
    scale = lax.rsqrt(squares * (1.0 / (inner * columns)) + epsilon)
    for k, value in enumerate(values):
        lanes = aligned(jnp.bitwise_xor(b, k), columns)
        state[:, lanes] = value
        normed[:, lanes] = (value * scale * gain[:, lanes].astype(f32)).astype(bf16)
    start = lax.axis_index("ctx") * rows
    for r in range(rows):
        mine[r : r + 1] = state[pl.ds(start + r, 1)]
    x = normed[...]
    gated = jnp.dot(x, gate[0], preferred_element_type=f32)
    lifted = jnp.dot(x, up[0], preferred_element_type=f32)
    active = (gated / (1.0 + jnp.exp(-gated)) * lifted).astype(bf16)
    held[...] = jnp.dot(active, down[0], preferred_element_type=f32)
    for s in range(shards):
        for j in range(held.shape[1] // LANES):
            dense[s, j * rows : (j + 1) * rows] = held[
                s * rows : (s + 1) * rows, j * LANES : (j + 1) * LANES
            ]
    out[...] = dense[...].astype(bf16)


def route(rows, ids, weights, out):
    chosen, weight = ids[...], weights[...]
    line = lax.broadcasted_iota(jnp.int32, out.shape[1:], 0)
    line = line - jnp.right_shift(line * (-(-65536 // rows)), 16) * rows
    for e in range(out.shape[0]):
        share = jnp.sum(jnp.where(chosen == e, weight, 0.0), axis=1, keepdims=True)
        block = jnp.zeros(out.shape[1:], f32)
        for r in range(rows):
            block = jnp.where(line == r, share[r : r + 1], block)
        out[e] = block


def combine(rows, state, back, routed, out, total):
    total[...] = sum(back[e].astype(f32) * routed[e] for e in range(back.shape[0]))
    for j in range(state.shape[1] // LANES):
        lanes = slice(j * LANES, (j + 1) * LANES)
        out[:, lanes] = (state[:, lanes] + total[j * rows : (j + 1) * rows]).astype(bf16)


def local(
    queries,
    cache_keys,
    cache_values,
    new_keys,
    new_values,
    cache_lengths,
    residual_in,
    out_weight,
    norm_gain,
    expert_gate,
    expert_up,
    expert_down,
    expert_ids,
    expert_weights,
):
    shards = lax.axis_size("ctx")
    outer = KV_HEADS
    inner = shards // outer
    rows, width = residual_in.shape
    cache = cache_keys.shape[0]
    count = -(-shards * rows // 16) * 16
    step = out_weight.shape[0]
    heads = max(1, step // HEAD_DIM)
    columns = width // inner
    lines = rows * width // LANES

    def shape(dims, dtype=bf16):
        return jax.ShapeDtypeStruct(dims, dtype)

    def outward(x, k):
        pairs = [(i, ((i // inner) ^ k) * inner + i % inner) for i in range(shards)]
        return lax.ppermute(x, "ctx", pairs)

    def inward(x, k):
        pairs = [(i, i // inner * inner + ((i % inner) ^ k)) for i in range(shards)]
        return lax.ppermute(x, "ctx", pairs)

    per_row = rows * GROUP
    span_lines = -(-(per_row + 2 * rows + 1) // 16) * 16
    pick, token = call(
        functools.partial(plan, outer, inner, rows, count),
        [shape((GROUP * count, shards * per_row)), shape((8, LANES), f32)],
        (),
        grant=max(4, count // 12),
    )
    spans = call(
        functools.partial(pack_span, outer, inner, rows),
        [shape((span_lines, HEAD_DIM))] * outer,
        (token, cache_lengths, new_keys, new_values, queries),
        [pltpu.VMEM((span_lines, HEAD_DIM), f32)],
    )
    spans = [spans[0]] + [outward(spans[k], k) for k in range(1, outer)]
    caches = call(
        functools.partial(pack_cache, outer, inner),
        [shape((2 * cache, HEAD_DIM))] * outer,
        (cache_keys, cache_values),
    )
    caches = [caches[0]] + [outward(caches[k], k) for k in range(1, outer)]
    wanted = call(
        functools.partial(collect, outer, rows),
        shape((outer * per_row, HEAD_DIM)),
        spans,
        [pltpu.VMEM((outer * per_row, HEAD_DIM), f32)],
    )
    wanted = [wanted] + [inward(wanted, k) for k in range(1, inner)]

    chunks = call(
        functools.partial(attend, outer, inner, rows, count, heads, step),
        [shape((heads * count, 2 * HEAD_DIM))] * inner,
        (pick, *spans, *caches, *wanted),
        [
            pltpu.VMEM((outer * span_lines, HEAD_DIM), f32),
            pltpu.VMEM((GROUP * count, 2 * HEAD_DIM), bf16),
        ],
        grant=max(8, count // 6),
    )
    chunks = [chunks[0]] + [inward(chunks[k], k) for k in range(1, inner)]

    if step < HEAD_DIM:
        at = lax.rem(lax.axis_index("ctx") * step, HEAD_DIM)
        out_weight = lax.dynamic_update_slice(
            jnp.zeros((HEAD_DIM, width), out_weight.dtype), out_weight, (at, 0)
        )
    kept, *parts = call(
        functools.partial(project, inner, rows, count, heads),
        [shape((count, columns), f32)] + [shape((count, columns))] * (inner - 1),
        (*chunks, out_weight, residual_in),
        [pltpu.VMEM((count, width), f32)],
        grant=max(4, count // 12),
    )
    parts = [inward(parts[k - 1], k) for k in range(1, inner)]
    both = [shape((count, columns), f32), shape((count, columns))]
    kept, sent = call(add_up, both, (kept, *parts))
    k = 1
    while k < outer:
        kept, sent = call(add_up, both, (kept, outward(sent, k)))
        k *= 2
    pieces = [kept] + [inward(sent, k) for k in range(1, inner)]

    results, state = call(
        functools.partial(expert, inner, rows, shards),
        [shape((shards, lines, LANES)), shape((rows, width), f32)],
        (expert_gate, expert_up, expert_down, norm_gain.reshape(1, width), *pieces),
        [
            pltpu.VMEM((count, width), f32),
            pltpu.VMEM((count, width), bf16),
            pltpu.VMEM((count, width), f32),
            pltpu.VMEM((shards, lines, LANES), f32),
        ],
        grant=max(8, count // 6),
    )
    back = lax.all_to_all(results, "ctx", split_axis=0, concat_axis=0, tiled=True)
    routed = call(
        functools.partial(route, rows),
        shape((shards, lines, LANES), f32),
        (expert_ids, expert_weights),
        flops=10**7,
    )
    return call(
        functools.partial(combine, rows),
        shape((rows, width)),
        (state, back, routed),
        [pltpu.VMEM((lines, LANES), f32)],
    )


def solution(mesh):
    placed = (
        P(("groups", "ctx"), None),
        P(("groups", "ctx"), None),
        P(("groups", "ctx"), None),
        P(("groups", "ctx"), None),
        P(("groups", "ctx"), None),
        P(("groups", "ctx")),
        P(("groups", "ctx"), None),
        P("ctx", None),
        P(),
        P("ctx", None, None),
        P("ctx", None, None),
        P("ctx", None, None),
        P(("groups", "ctx"), None),
        P(("groups", "ctx"), None),
    )
    return jax.shard_map(
        local, mesh=mesh, in_specs=placed, out_specs=P(("groups", "ctx"), None), check_vma=False
    )
```

```python
import functools

import jax
import jax.numpy as jnp
from jax import lax
from jax.experimental import pallas as pl
from jax.experimental.pallas import tpu as pltpu
from jax.sharding import PartitionSpec as P


HEADS = 32
KV_HEADS = 4
HEAD_DIM = 128
GROUP = HEADS // KV_HEADS
LANES = 128

MASKED = -1e30
epsilon = 1e-06

f32, bf16 = jnp.float32, jnp.bfloat16
VMEM = pl.BlockSpec(memory_space=pltpu.VMEM)


def coordinates(inner):
    device = lax.axis_index("ctx")
    return device // inner, lax.rem(device, inner)


def call(body, outs, operands, scratch=(), grant=4, flops=10**9):
    return pl.pallas_call(
        body,
        out_shape=outs,
        in_specs=[VMEM] * len(operands),
        out_specs=jax.tree.map(lambda _: VMEM, outs),
        scratch_shapes=list(scratch),
        compiler_params=pltpu.CompilerParams(vmem_limit_bytes=grant << 20),
        cost_estimate=pl.CostEstimate(flops=flops, bytes_accessed=10**6, transcendentals=0),
    )(*operands)


def third(x, rows):
    return jnp.right_shift(x * (-(-65536 // rows)), 16)


def owners(position, half, rows):
    odd = (position >= half).astype(jnp.int32)
    rest = position - odd * half
    pair = third(rest, rows)
    return 2 * pair + odd, rest - pair * rows


def place(shard, half, rows):
    return jnp.bitwise_and(shard, 1) * half + jnp.right_shift(shard, 1) * rows


def aligned(index, size):
    return pl.ds(pl.multiple_of(index * size, size), size)


def pack_span(outer, inner, rows, lines, token, lengths, new_keys, new_values, queries, ids, weights, *refs):
    outs, (wide, routing) = refs[:outer], refs[outer:]
    a, _ = coordinates(inner)
    per_row = rows * GROUP
    live = lengths[...].astype(f32).reshape(1, 1)
    wide[...] = jnp.zeros_like(wide)
    wide[per_row + 2 * rows : per_row + 2 * rows + 1] = jnp.broadcast_to(live, (1, HEAD_DIM))
    weight = weights[...]
    high = weight.astype(bf16).astype(f32)
    routing[...] = jnp.zeros_like(routing)
    for i, part in enumerate((ids[...].astype(f32), high, weight - high)):
        routing[8 * i : 8 * i + rows] = part
    top = ids.shape[1]
    lane = lax.broadcasted_iota(jnp.int32, (top, HEAD_DIM), 1)
    turn = lax.broadcasted_iota(jnp.int32, (top, HEAD_DIM), 0)
    copies = jnp.where(lax.rem(lane, top) == turn, 1.0, 0.0).astype(bf16)
    repeated = jnp.dot(routing[...].astype(bf16), copies, preferred_element_type=f32)
    lane = lax.broadcasted_iota(jnp.int32, (8, HEAD_DIM), 1)
    row = lax.broadcasted_iota(jnp.int32, (8, HEAD_DIM), 0)
    inside = (lane >= row * top) & (lane < row * top + top)
    for i in range(3):
        wide[lines + i : lines + i + 1] = jnp.sum(
            jnp.where(inside, repeated[8 * i : 8 * i + 8], 0.0), axis=0, keepdims=True
        )
    for k in range(outer):
        head = jnp.bitwise_xor(a, k)
        lanes = aligned(head, HEAD_DIM)
        block = queries[:, aligned(head, GROUP * HEAD_DIM)].astype(f32)
        for g in range(GROUP):
            wide[g * rows : (g + 1) * rows] = block[:, g * HEAD_DIM : (g + 1) * HEAD_DIM]
        wide[per_row : per_row + rows] = new_keys[:, lanes].astype(f32)
        wide[per_row + rows : per_row + 2 * rows] = new_values[:, lanes].astype(f32)
        outs[k][...] = wide[...].astype(bf16)


def pack_cache(outer, inner, keys, values, *outs):
    a, _ = coordinates(inner)
    cache = keys.shape[0]
    for k in range(outer):
        lanes = aligned(jnp.bitwise_xor(a, k), HEAD_DIM)
        outs[k][0:cache] = keys[:, lanes]
        outs[k][cache:] = values[:, lanes]


def plan(outer, inner, rows, count, pick, token):
    a, b = coordinates(inner)
    per_row = rows * GROUP
    position = lax.broadcasted_iota(jnp.int32, (count, 1), 0)
    owner, row = owners(position, count // 2, rows)
    at_a = jnp.bitwise_xor(jnp.right_shift(owner, inner.bit_length() - 1), a)
    at_b = jnp.bitwise_xor(jnp.bitwise_and(owner, inner - 1), b)
    source = (at_b * outer + at_a) * per_row + row
    source = jnp.where(owner < outer * inner, source, -per_row)
    column = lax.broadcasted_iota(jnp.int32, (count, pick.shape[1]), 1)
    for g in range(GROUP):
        pick[g * count : (g + 1) * count] = jnp.where(
            column == source + g * rows, 1.0, 0.0
        ).astype(bf16)
    token[...] = jnp.zeros_like(token)


def collect(outer, rows, lines, *refs):
    spans, out, wide = refs[:outer], refs[outer], refs[outer + 1]
    per_row = rows * GROUP
    for k in range(outer):
        block = spans[k][...].astype(f32)
        wide[k * per_row : (k + 1) * per_row] = block[0:per_row]
        for i in range(3):
            at = outer * per_row + i * outer + k
            wide[at : at + 1] = block[lines + i : lines + i + 1]
    out[...] = wide[...].astype(bf16)


def attend(outer, inner, rows, lines, count, heads, step, *refs):
    pick, spans, caches = refs[0], refs[1 : outer + 1], refs[outer + 1 : 2 * outer + 1]
    queries, refs = refs[2 * outer + 1 : 2 * outer + 1 + inner], refs[2 * outer + 1 + inner :]
    outs, (fresh, parts) = refs[:inner], refs[inner:]
    a, b = coordinates(inner)
    cache = caches[0].shape[0] // 2
    per_row = rows * GROUP
    gathered = jnp.concatenate([block[0 : outer * per_row] for block in queries], 0)
    wanted = jnp.dot(pick[...], gathered, preferred_element_type=f32).astype(bf16)

    def score(keys, usable):
        s = lax.dot_general(
            wanted, keys, (((1,), (1,)), ((), ())), preferred_element_type=f32
        ) * HEAD_DIM ** (-0.5)
        return jnp.where(usable, s.reshape((GROUP, count, keys.shape[0])), MASKED)

    fresh[...] = jnp.zeros_like(fresh)
    owner, row = owners(lax.broadcasted_iota(jnp.int32, (count, 1), 0), count // 2, rows)
    position = owner * rows + row
    slot = lax.broadcasted_iota(jnp.int32, (count, outer * lines), 1)
    reach = jnp.full((count, outer * lines), -1, jnp.int32)
    lives = []
    for k in range(outer):
        block = spans[k][0:lines].astype(f32)
        lives.append(block[per_row + 2 * rows : per_row + 2 * rows + 1, 0:1])
        first = k * lines + per_row
        fresh[first : first + rows] = block[per_row + rows : per_row + 2 * rows]
        start = rows * (jnp.bitwise_xor(a, k) * inner + b)
        inside = (slot >= first) & (slot < first + rows)
        reach = jnp.where(inside, position - start - (slot - first), reach)
    keys = [jnp.concatenate([block[0:lines] for block in spans], 0)]
    values = [fresh[...].astype(bf16)]
    usable = [(reach >= 0)[None]]
    index = lax.broadcasted_iota(jnp.int32, (count, cache), 1).astype(f32)
    for k in range(outer):
        keys.append(caches[k][0:cache])
        values.append(caches[k][cache:])
        usable.append(((lives[k] - index) > 0.0)[None])
    scores = [score(key, ok) for key, ok in zip(keys, usable)]
    largest = functools.reduce(
        jnp.maximum, [jnp.max(s, axis=-1, keepdims=True) for s in scores]
    )
    largest = largest.astype(bf16).astype(f32)
    total = jnp.zeros((GROUP, count, 1), f32)
    summed = jnp.zeros((GROUP * count, HEAD_DIM), f32)
    for s, ok, value in zip(scores, usable, values):
        e = jnp.where(ok, jnp.exp(s - largest), 0.0)
        total = total + jnp.sum(e, axis=-1, keepdims=True)
        summed = summed + jnp.dot(
            e.reshape(GROUP * count, value.shape[0]).astype(bf16),
            value,
            preferred_element_type=f32,
        )
    total = total.reshape(GROUP * count, 1)
    high = total.astype(bf16).astype(f32)
    lane = lax.broadcasted_iota(jnp.int32, (GROUP * count, HEAD_DIM), 1)
    stats = jnp.where(
        lane == 0,
        largest.reshape(GROUP * count, 1),
        jnp.where(lane == 1, high, total - high),
    )
    parts[:, 0:HEAD_DIM] = summed.astype(bf16)
    parts[:, HEAD_DIM:] = stats.astype(bf16)
    for k in range(inner):
        first = jnp.right_shift(jnp.bitwise_xor(b, k) * step, HEAD_DIM.bit_length() - 1)
        outs[k][...] = parts[pl.ds(pl.multiple_of(first * count, 16), heads * count)]


def project(inner, rows, count, heads, *refs):
    chunks, (weight, residual), refs = refs[:inner], refs[inner : inner + 2], refs[inner + 2 :]
    own, outs, total = refs[0], refs[1:inner], refs[inner]
    _, b = coordinates(inner)
    stats = [chunk[:, HEAD_DIM:].astype(f32) for chunk in chunks]
    largest = functools.reduce(jnp.maximum, [s[:, 0:1] for s in stats])
    scales = [jnp.exp(s[:, 0:1] - largest) for s in stats]
    denominator = sum(w * (s[:, 1:2] + s[:, 2:3]) for w, s in zip(scales, stats))
    joined = sum(
        chunk[:, 0:HEAD_DIM].astype(f32) * (w / denominator)
        for w, chunk in zip(scales, chunks)
    ).astype(bf16)
    total[...] = sum(
        jnp.dot(
            joined[h * count : (h + 1) * count],
            weight[h * HEAD_DIM : (h + 1) * HEAD_DIM],
            preferred_element_type=f32,
        )
        for h in range(heads)
    )
    start = place(lax.axis_index("ctx"), count // 2, rows)
    added = residual[...].astype(f32)
    for r in range(rows):
        row = pl.ds(start + r, 1)
        total[row] = total[row] + added[r : r + 1]
    columns = own.shape[1]
    own[...] = total[:, aligned(b, columns)]
    for k in range(1, inner):
        outs[k - 1][...] = total[:, aligned(jnp.bitwise_xor(b, k), columns)].astype(bf16)


def add_up(own, *refs):
    others, (kept, sent) = refs[:-2], refs[-2:]
    partial = own[...]
    for other in others:
        partial = partial + other[...].astype(f32)
    kept[...] = partial
    sent[...] = partial.astype(bf16)


def route(outer, inner, rows, count, top, *refs):
    blocks, out = refs[:-1], refs[-1]
    a, b = coordinates(inner)
    expert = lax.axis_index("ctx").astype(f32)
    lane = lax.broadcasted_iota(jnp.int32, (outer, HEAD_DIM), 1)
    for m in range(inner):
        info = blocks[m][outer * rows * GROUP :].astype(f32)
        named, high, low = (info[i * outer : (i + 1) * outer] for i in range(3))
        weight = jnp.where(named == expert, high + low, 0.0)
        for r in range(rows):
            inside = (lane >= r * top) & (lane < r * top + top)
            share = jnp.sum(jnp.where(inside, weight, 0.0), axis=1, keepdims=True)
            share = jnp.broadcast_to(share, (outer, LANES))
            for k in range(outer):
                shard = jnp.bitwise_xor(a, k) * inner + jnp.bitwise_xor(b, m)
                out[pl.ds(place(shard, count // 2, rows) + r, 1)] = share[k : k + 1]


def expert(inner, rows, gate, up, down, gain, weights, *refs):
    pieces, (kept, sent, mine, state, normed, held) = refs[:inner], refs[inner:]
    _, b = coordinates(inner)
    columns = pieces[0].shape[1]
    half = kept.shape[0]
    values = [piece[...].astype(f32) for piece in pieces]
    squares = sum(jnp.sum(v * v, axis=1, keepdims=True) for v in values)
    scale = lax.rsqrt(squares * (1.0 / (inner * columns)) + epsilon)
    for k, value in enumerate(values):
        lanes = aligned(jnp.bitwise_xor(b, k), columns)
        state[:, lanes] = value
        normed[:, lanes] = (value * scale * gain[:, lanes].astype(f32)).astype(bf16)
    start = place(lax.axis_index("ctx"), half, rows)
    for r in range(rows):
        mine[r : r + 1] = state[pl.ds(start + r, 1)]
    x = normed[...]
    gated = jnp.dot(x, gate[0], preferred_element_type=f32)
    lifted = jnp.dot(x, up[0], preferred_element_type=f32)
    active = (gated / (1.0 + jnp.exp(-gated)) * lifted).astype(bf16)
    held[...] = jnp.dot(active, down[0], preferred_element_type=f32) * weights[:, 0:1]
    odd = jnp.bitwise_and(b, 1)
    kept[...] = held[aligned(odd, half)]
    sent[...] = held[aligned(1 - odd, half)].astype(bf16)


def join(rows, kept, other, out, total, dense):
    total[...] = kept[...] + other[...].astype(f32)
    for t in range(out.shape[0]):
        for j in range(total.shape[1] // LANES):
            dense[t, j * rows : (j + 1) * rows] = total[
                t * rows : (t + 1) * rows, j * LANES : (j + 1) * LANES
            ]
    out[...] = dense[...].astype(bf16)


def combine(rows, state, back, out, total):
    total[...] = sum(back[t].astype(f32) for t in range(back.shape[0]))
    for j in range(state.shape[1] // LANES):
        lanes = slice(j * LANES, (j + 1) * LANES)
        out[:, lanes] = (state[:, lanes] + total[j * rows : (j + 1) * rows]).astype(bf16)


def local(
    queries,
    cache_keys,
    cache_values,
    new_keys,
    new_values,
    cache_lengths,
    residual_in,
    out_weight,
    norm_gain,
    expert_gate,
    expert_up,
    expert_down,
    expert_ids,
    expert_weights,
):
    shards = lax.axis_size("ctx")
    outer = KV_HEADS
    inner = shards // outer
    rows, width = residual_in.shape
    cache = cache_keys.shape[0]
    half = -(-shards // 2 * rows // 8) * 8
    count = 2 * half
    top = expert_ids.shape[1]
    step = out_weight.shape[0]
    heads = max(1, step // HEAD_DIM)
    columns = width // inner
    lines = rows * width // LANES

    def shape(dims, dtype=bf16):
        return jax.ShapeDtypeStruct(dims, dtype)

    def outward(x, k):
        pairs = [(i, ((i // inner) ^ k) * inner + i % inner) for i in range(shards)]
        return lax.ppermute(x, "ctx", pairs)

    def inward(x, k):
        pairs = [(i, i // inner * inner + ((i % inner) ^ k)) for i in range(shards)]
        return lax.ppermute(x, "ctx", pairs)

    def exchange(move, blocks):
        moved = [blocks[0]]
        for k in range(1, len(blocks)):
            moved.append(move(blocks[k], k))
        return moved

    per_row = rows * GROUP
    span_lines = -(-(per_row + 2 * rows + 1) // 16) * 16
    asked_lines = outer * per_row + -(-3 * outer // 8) * 8
    pick, token = call(
        functools.partial(plan, outer, inner, rows, count),
        [shape((GROUP * count, shards * per_row)), shape((8, LANES), f32)],
        (),
        grant=max(4, count // 12),
    )
    spans = call(
        functools.partial(pack_span, outer, inner, rows, span_lines),
        [shape((span_lines + 8, HEAD_DIM))] * outer,
        (token, cache_lengths, new_keys, new_values, queries, expert_ids, expert_weights),
        [pltpu.VMEM((span_lines + 8, HEAD_DIM), f32), pltpu.VMEM((24, top), f32)],
    )
    spans = exchange(outward, spans)
    caches = call(
        functools.partial(pack_cache, outer, inner),
        [shape((2 * cache, HEAD_DIM))] * outer,
        (cache_keys, cache_values),
    )
    caches = exchange(outward, caches)
    wanted = call(
        functools.partial(collect, outer, rows, span_lines),
        shape((asked_lines, HEAD_DIM)),
        spans,
        [pltpu.VMEM((asked_lines, HEAD_DIM), f32)],
    )
    wanted = exchange(inward, [wanted] * inner)

    chunks = call(
        functools.partial(attend, outer, inner, rows, span_lines, count, heads, step),
        [shape((heads * count, 2 * HEAD_DIM))] * inner,
        (pick, *spans, *caches, *wanted),
        [
            pltpu.VMEM((outer * span_lines, HEAD_DIM), f32),
            pltpu.VMEM((GROUP * count, 2 * HEAD_DIM), bf16),
        ],
        grant=max(8, count // 6),
    )
    chunks = exchange(inward, chunks)

    if step < HEAD_DIM:
        at = lax.rem(lax.axis_index("ctx") * step, HEAD_DIM)
        out_weight = lax.dynamic_update_slice(
            jnp.zeros((HEAD_DIM, width), out_weight.dtype), out_weight, (at, 0)
        )
    kept, *parts = call(
        functools.partial(project, inner, rows, count, heads),
        [shape((count, columns), f32)] + [shape((count, columns))] * (inner - 1),
        (*chunks, out_weight, residual_in),
        [pltpu.VMEM((count, width), f32)],
        grant=max(4, count // 12),
    )
    parts = exchange(inward, [None] + parts)[1:]
    both = [shape((count, columns), f32), shape((count, columns))]
    kept, sent = call(add_up, both, (kept, *parts))
    k = 1
    while k < outer:
        kept, sent = call(add_up, both, (kept, outward(sent, k)))
        k *= 2
    pieces = [kept] + exchange(inward, [sent] * inner)[1:]

    weights = call(
        functools.partial(route, outer, inner, rows, count, top),
        shape((count, LANES), f32),
        wanted,
        flops=10**7,
    )
    kept, sent, state = call(
        functools.partial(expert, inner, rows),
        [shape((half, width), f32), shape((half, width)), shape((rows, width), f32)],
        (expert_gate, expert_up, expert_down, norm_gain.reshape(1, width), weights, *pieces),
        [
            pltpu.VMEM((count, width), f32),
            pltpu.VMEM((count, width), bf16),
            pltpu.VMEM((count, width), f32),
        ],
        grant=max(8, count // 6),
    )
    sums = call(
        functools.partial(join, rows),
        shape((shards // 2, lines, LANES)),
        (kept, inward(sent, 1)),
        [pltpu.VMEM((half, width), f32), pltpu.VMEM((shards // 2, lines, LANES), f32)],
        grant=max(4, count // 12),
    )
    parity = [[2 * t + odd for t in range(shards // 2)] for odd in range(2)]
    back = lax.all_to_all(
        sums, "ctx", split_axis=0, concat_axis=0, tiled=True, axis_index_groups=parity
    )
    return call(
        functools.partial(combine, rows),
        shape((rows, width)),
        (state, back),
        [pltpu.VMEM((lines, LANES), f32)],
    )


def solution(mesh):
    placed = (
        P(("groups", "ctx"), None),
        P(("groups", "ctx"), None),
        P(("groups", "ctx"), None),
        P(("groups", "ctx"), None),
        P(("groups", "ctx"), None),
        P(("groups", "ctx")),
        P(("groups", "ctx"), None),
        P("ctx", None),
        P(),
        P("ctx", None, None),
        P("ctx", None, None),
        P("ctx", None, None),
        P(("groups", "ctx"), None),
        P(("groups", "ctx"), None),
    )
    return jax.shard_map(
        local, mesh=mesh, in_specs=placed, out_specs=P(("groups", "ctx"), None), check_vma=False
    )
```

```python
import functools

import jax
import jax.numpy as jnp
from jax import lax
from jax.experimental import pallas as pl
from jax.experimental.pallas import tpu as pltpu
from jax.sharding import PartitionSpec as P


HEADS = 32
KV_HEADS = 4
HEAD_DIM = 128
GROUP = HEADS // KV_HEADS
LANES = 128

MASKED = -1e30
epsilon = 1e-06

f32, bf16 = jnp.float32, jnp.bfloat16
VMEM = pl.BlockSpec(memory_space=pltpu.VMEM)


def coordinates(inner):
    device = lax.axis_index("ctx")
    return device // inner, lax.rem(device, inner)


def call(body, outs, operands, scratch=(), grant=4, flops=10**9):
    return pl.pallas_call(
        body,
        out_shape=outs,
        in_specs=[VMEM] * len(operands),
        out_specs=jax.tree.map(lambda _: VMEM, outs),
        scratch_shapes=list(scratch),
        compiler_params=pltpu.CompilerParams(vmem_limit_bytes=grant << 20),
        cost_estimate=pl.CostEstimate(flops=flops, bytes_accessed=10**6, transcendentals=0),
    )(*operands)


def third(x, rows):
    return jnp.right_shift(x * (-(-65536 // rows)), 16)


def owners(position, half, rows):
    odd = (position >= half).astype(jnp.int32)
    rest = position - odd * half
    pair = third(rest, rows)
    return 2 * pair + odd, rest - pair * rows


def place(shard, half, rows):
    return jnp.bitwise_and(shard, 1) * half + jnp.right_shift(shard, 1) * rows


def stat_lines(lines):
    starts = range(0, lines, LANES)
    return [(s, min(LANES, lines - s), lines + 16 * i) for i, s in enumerate(starts)]


def selection():
    line = lax.broadcasted_iota(jnp.int32, (16, LANES), 0)
    lane = lax.broadcasted_iota(jnp.int32, (16, LANES), 1)
    return jnp.where(line == lane, 1.0, 0.0).astype(bf16)


def aligned(index, size):
    return pl.ds(pl.multiple_of(index * size, size), size)


def pack_span(outer, inner, rows, lines, token, lengths, new_keys, new_values, queries, ids, weights, *refs):
    outs, (wide, routing) = refs[:outer], refs[outer:]
    a, _ = coordinates(inner)
    per_row = rows * GROUP
    live = lengths[...].astype(f32).reshape(1, 1)
    wide[...] = jnp.zeros_like(wide)
    wide[per_row + 2 * rows : per_row + 2 * rows + 1] = jnp.broadcast_to(live, (1, HEAD_DIM))
    weight = weights[...]
    high = weight.astype(bf16).astype(f32)
    routing[...] = jnp.zeros_like(routing)
    for i, part in enumerate((ids[...].astype(f32), high, weight - high)):
        routing[8 * i : 8 * i + rows] = part
    top = ids.shape[1]
    lane = lax.broadcasted_iota(jnp.int32, (top, HEAD_DIM), 1)
    turn = lax.broadcasted_iota(jnp.int32, (top, HEAD_DIM), 0)
    copies = jnp.where(lax.rem(lane, top) == turn, 1.0, 0.0).astype(bf16)
    repeated = jnp.dot(routing[...].astype(bf16), copies, preferred_element_type=f32)
    lane = lax.broadcasted_iota(jnp.int32, (8, HEAD_DIM), 1)
    row = lax.broadcasted_iota(jnp.int32, (8, HEAD_DIM), 0)
    inside = (lane >= row * top) & (lane < row * top + top)
    for i in range(3):
        wide[lines + i : lines + i + 1] = jnp.sum(
            jnp.where(inside, repeated[8 * i : 8 * i + 8], 0.0), axis=0, keepdims=True
        )
    for k in range(outer):
        head = jnp.bitwise_xor(a, k)
        lanes = aligned(head, HEAD_DIM)
        block = queries[:, aligned(head, GROUP * HEAD_DIM)].astype(f32)
        for g in range(GROUP):
            wide[g * rows : (g + 1) * rows] = block[:, g * HEAD_DIM : (g + 1) * HEAD_DIM]
        wide[per_row : per_row + rows] = new_keys[:, lanes].astype(f32)
        wide[per_row + rows : per_row + 2 * rows] = new_values[:, lanes].astype(f32)
        outs[k][...] = wide[...].astype(bf16)


def pack_cache(outer, inner, keys, values, *outs):
    a, _ = coordinates(inner)
    cache = keys.shape[0]
    for k in range(outer):
        lanes = aligned(jnp.bitwise_xor(a, k), HEAD_DIM)
        outs[k][0:cache] = keys[:, lanes]
        outs[k][cache:] = values[:, lanes]


def plan(outer, inner, rows, count, pick, token):
    a, b = coordinates(inner)
    per_row = rows * GROUP
    position = lax.broadcasted_iota(jnp.int32, (count, 1), 0)
    owner, row = owners(position, count // 2, rows)
    at_a = jnp.bitwise_xor(jnp.right_shift(owner, inner.bit_length() - 1), a)
    at_b = jnp.bitwise_xor(jnp.bitwise_and(owner, inner - 1), b)
    source = (at_b * outer + at_a) * per_row + row
    source = jnp.where(owner < outer * inner, source, -per_row)
    column = lax.broadcasted_iota(jnp.int32, (count, pick.shape[1]), 1)
    for g in range(GROUP):
        pick[g * count : (g + 1) * count] = jnp.where(
            column == source + g * rows, 1.0, 0.0
        ).astype(bf16)
    token[...] = jnp.zeros_like(token)


def collect(outer, rows, lines, *refs):
    spans, out, wide = refs[:outer], refs[outer], refs[outer + 1]
    per_row = rows * GROUP
    for k in range(outer):
        block = spans[k][...].astype(f32)
        wide[k * per_row : (k + 1) * per_row] = block[0:per_row]
        for i in range(3):
            at = outer * per_row + i * outer + k
            wide[at : at + 1] = block[lines + i : lines + i + 1]
    out[...] = wide[...].astype(bf16)


def attend(outer, inner, rows, lines, count, heads, step, *refs):
    pick, spans, caches = refs[0], refs[1 : outer + 1], refs[outer + 1 : 2 * outer + 1]
    queries, refs = refs[2 * outer + 1 : 2 * outer + 1 + inner], refs[2 * outer + 1 + inner :]
    outs, (fresh, parts) = refs[:inner], refs[inner:]
    a, b = coordinates(inner)
    cache = caches[0].shape[0] // 2
    per_row = rows * GROUP
    gathered = jnp.concatenate([block[0 : outer * per_row] for block in queries], 0)
    wanted = jnp.dot(pick[...], gathered, preferred_element_type=f32).astype(bf16)

    def score(keys, usable):
        s = lax.dot_general(
            wanted, keys, (((1,), (1,)), ((), ())), preferred_element_type=f32
        ) * HEAD_DIM ** (-0.5)
        return jnp.where(usable, s.reshape((GROUP, count, keys.shape[0])), MASKED)

    fresh[...] = jnp.zeros_like(fresh)
    owner, row = owners(lax.broadcasted_iota(jnp.int32, (count, 1), 0), count // 2, rows)
    position = owner * rows + row
    slot = lax.broadcasted_iota(jnp.int32, (count, outer * lines), 1)
    reach = jnp.full((count, outer * lines), -1, jnp.int32)
    lives = []
    for k in range(outer):
        block = spans[k][0:lines].astype(f32)
        lives.append(block[per_row + 2 * rows : per_row + 2 * rows + 1, 0:1])
        first = k * lines + per_row
        fresh[first : first + rows] = block[per_row + rows : per_row + 2 * rows]
        start = rows * (jnp.bitwise_xor(a, k) * inner + b)
        inside = (slot >= first) & (slot < first + rows)
        reach = jnp.where(inside, position - start - (slot - first), reach)
    keys = [jnp.concatenate([block[0:lines] for block in spans], 0)]
    values = [fresh[...].astype(bf16)]
    usable = [(reach >= 0)[None]]
    index = lax.broadcasted_iota(jnp.int32, (count, cache), 1).astype(f32)
    for k in range(outer):
        keys.append(caches[k][0:cache])
        values.append(caches[k][cache:])
        usable.append(((lives[k] - index) > 0.0)[None])
    scores = [score(key, ok) for key, ok in zip(keys, usable)]
    largest = functools.reduce(
        jnp.maximum, [jnp.max(s, axis=-1, keepdims=True) for s in scores]
    )
    largest = largest.astype(bf16).astype(f32)
    total = jnp.zeros((GROUP, count, 1), f32)
    summed = jnp.zeros((GROUP * count, HEAD_DIM), f32)
    for s, ok, value in zip(scores, usable, values):
        e = jnp.where(ok, jnp.exp(s - largest), 0.0)
        total = total + jnp.sum(e, axis=-1, keepdims=True)
        summed = summed + jnp.dot(
            e.reshape(GROUP * count, value.shape[0]).astype(bf16),
            value,
            preferred_element_type=f32,
        )
    total = total.reshape(GROUP * count, 1)
    high = total.astype(bf16).astype(f32)
    lane = lax.broadcasted_iota(jnp.int32, (GROUP * count, HEAD_DIM), 1)
    stats = jnp.where(
        lane == 0,
        largest.reshape(GROUP * count, 1),
        jnp.where(lane == 1, high, total - high),
    )
    parts[:, 0:HEAD_DIM] = summed.astype(bf16)
    parts[:, HEAD_DIM:] = stats.astype(bf16)
    for k in range(inner):
        first = jnp.right_shift(jnp.bitwise_xor(b, k) * step, HEAD_DIM.bit_length() - 1)
        first, lines = pl.multiple_of(first * count, 16), heads * count
        outs[k][0:lines] = parts[pl.ds(first, lines), 0:HEAD_DIM]
        outs[k][lines:] = jnp.zeros((outs[k].shape[0] - lines, LANES), bf16)
        for start, size, at in stat_lines(lines):
            block = parts[pl.ds(pl.multiple_of(first + start, 16), size), HEAD_DIM:]
            outs[k][at : at + 16, 0:size] = lax.dot_general(
                selection(), block, (((1,), (1,)), ((), ())), preferred_element_type=f32
            ).astype(bf16)


def project(inner, rows, count, heads, *refs):
    chunks, (weight, residual), refs = refs[:inner], refs[inner : inner + 2], refs[inner + 2 :]
    own, outs, total = refs[0], refs[1:inner], refs[inner]
    _, b = coordinates(inner)
    lines = heads * count
    stats = [
        jnp.concatenate(
            [
                lax.dot_general(
                    chunk[at : at + 16, 0:size],
                    selection(),
                    (((0,), (0,)), ((), ())),
                    preferred_element_type=f32,
                )
                for _, size, at in stat_lines(lines)
            ],
            0,
        )
        for chunk in chunks
    ]
    largest = functools.reduce(jnp.maximum, [s[:, 0:1] for s in stats])
    scales = [jnp.exp(s[:, 0:1] - largest) for s in stats]
    denominator = sum(w * (s[:, 1:2] + s[:, 2:3]) for w, s in zip(scales, stats))
    joined = sum(
        chunk[0:lines].astype(f32) * (w / denominator)
        for w, chunk in zip(scales, chunks)
    ).astype(bf16)
    total[...] = sum(
        jnp.dot(
            joined[h * count : (h + 1) * count],
            weight[h * HEAD_DIM : (h + 1) * HEAD_DIM],
            preferred_element_type=f32,
        )
        for h in range(heads)
    )
    start = place(lax.axis_index("ctx"), count // 2, rows)
    added = residual[...].astype(f32)
    for r in range(rows):
        row = pl.ds(start + r, 1)
        total[row] = total[row] + added[r : r + 1]
    columns = own.shape[1]
    own[...] = total[:, aligned(b, columns)]
    for k in range(1, inner):
        outs[k - 1][...] = total[:, aligned(jnp.bitwise_xor(b, k), columns)].astype(bf16)


def add_up(own, *refs):
    others, (kept, sent) = refs[:-2], refs[-2:]
    partial = own[...]
    for other in others:
        partial = partial + other[...].astype(f32)
    kept[...] = partial
    sent[...] = partial.astype(bf16)


def route(outer, inner, rows, count, top, *refs):
    blocks, out = refs[:-1], refs[-1]
    a, b = coordinates(inner)
    expert = lax.axis_index("ctx").astype(f32)
    lane = lax.broadcasted_iota(jnp.int32, (outer, HEAD_DIM), 1)
    for m in range(inner):
        info = blocks[m][outer * rows * GROUP :].astype(f32)
        named, high, low = (info[i * outer : (i + 1) * outer] for i in range(3))
        weight = jnp.where(named == expert, high + low, 0.0)
        for r in range(rows):
            inside = (lane >= r * top) & (lane < r * top + top)
            share = jnp.sum(jnp.where(inside, weight, 0.0), axis=1, keepdims=True)
            share = jnp.broadcast_to(share, (outer, LANES))
            for k in range(outer):
                shard = jnp.bitwise_xor(a, k) * inner + jnp.bitwise_xor(b, m)
                out[pl.ds(place(shard, count // 2, rows) + r, 1)] = share[k : k + 1]


def begin(inner, gate, up, gain, *refs):
    pieces, (gated, lifted, squares) = refs[:-3], refs[-3:]
    _, b = coordinates(inner)
    columns = pieces[0].shape[1]
    total, sums = jnp.zeros(squares.shape, f32), [0.0, 0.0]
    for k, piece in enumerate(pieces):
        lanes = aligned(jnp.bitwise_xor(b, k), columns)
        value = piece[...].astype(f32)
        total = total + jnp.sum(value * value, axis=1, keepdims=True)
        x = (value * gain[:, lanes].astype(f32)).astype(bf16)
        for i, weight in enumerate((gate, up)):
            sums[i] = sums[i] + jnp.dot(x, weight[0, lanes], preferred_element_type=f32)
    gated[...], lifted[...] = sums
    squares[...] = total


def expert(inner, early, rows, gate, up, down, gain, weights, begun_gate, begun_up, begun, *refs):
    pieces, (kept, sent, mine, state, held) = refs[:inner], refs[inner:]
    _, b = coordinates(inner)
    columns = pieces[0].shape[1]
    half = kept.shape[0]
    squares, gated, lifted = begun[:, 0:1], begun_gate[...], begun_up[...]
    for k, piece in enumerate(pieces):
        lanes = aligned(jnp.bitwise_xor(b, k), columns)
        value = piece[...].astype(f32)
        state[:, lanes] = value
        if k >= early:
            squares = squares + jnp.sum(value * value, axis=1, keepdims=True)
            x = (value * gain[:, lanes].astype(f32)).astype(bf16)
            gated = gated + jnp.dot(x, gate[0, lanes], preferred_element_type=f32)
            lifted = lifted + jnp.dot(x, up[0, lanes], preferred_element_type=f32)
    scale = lax.rsqrt(squares * (1.0 / (inner * columns)) + epsilon)
    gated, lifted = gated * scale, lifted * scale
    start = place(lax.axis_index("ctx"), half, rows)
    for r in range(rows):
        mine[r : r + 1] = state[pl.ds(start + r, 1)]
    active = (gated / (1.0 + jnp.exp(-gated)) * lifted).astype(bf16)
    held[...] = jnp.dot(active, down[0], preferred_element_type=f32) * weights[:, 0:1]
    odd = jnp.bitwise_and(b, 1)
    kept[...] = held[aligned(odd, half)]
    sent[...] = held[aligned(1 - odd, half)].astype(bf16)


def join(rows, kept, other, out, total, dense):
    total[...] = kept[...] + other[...].astype(f32)
    for t in range(out.shape[0]):
        for j in range(total.shape[1] // LANES):
            dense[t, j * rows : (j + 1) * rows] = total[
                t * rows : (t + 1) * rows, j * LANES : (j + 1) * LANES
            ]
    out[...] = dense[...].astype(bf16)


def combine(rows, state, back, out, total):
    total[...] = sum(back[t].astype(f32) for t in range(back.shape[0]))
    for j in range(state.shape[1] // LANES):
        lanes = slice(j * LANES, (j + 1) * LANES)
        out[:, lanes] = (state[:, lanes] + total[j * rows : (j + 1) * rows]).astype(bf16)


def local(
    queries,
    cache_keys,
    cache_values,
    new_keys,
    new_values,
    cache_lengths,
    residual_in,
    out_weight,
    norm_gain,
    expert_gate,
    expert_up,
    expert_down,
    expert_ids,
    expert_weights,
):
    shards = lax.axis_size("ctx")
    outer = KV_HEADS
    inner = shards // outer
    rows, width = residual_in.shape
    cache = cache_keys.shape[0]
    half = -(-shards // 2 * rows // 8) * 8
    count = 2 * half
    top = expert_ids.shape[1]
    step = out_weight.shape[0]
    heads = max(1, step // HEAD_DIM)
    columns = width // inner
    lines = rows * width // LANES

    def shape(dims, dtype=bf16):
        return jax.ShapeDtypeStruct(dims, dtype)

    def outward(x, k):
        pairs = [(i, ((i // inner) ^ k) * inner + i % inner) for i in range(shards)]
        return lax.ppermute(x, "ctx", pairs)

    def inward(x, k):
        pairs = [(i, i // inner * inner + ((i % inner) ^ k)) for i in range(shards)]
        return lax.ppermute(x, "ctx", pairs)

    def exchange(move, blocks):
        moved = [blocks[0]]
        for k in range(1, len(blocks)):
            moved.append(move(blocks[k], k))
        return moved

    per_row = rows * GROUP
    span_lines = -(-(per_row + 2 * rows + 1) // 16) * 16
    asked_lines = outer * per_row + -(-3 * outer // 8) * 8
    pick, token = call(
        functools.partial(plan, outer, inner, rows, count),
        [shape((GROUP * count, shards * per_row)), shape((8, LANES), f32)],
        (),
        grant=max(4, count // 12),
    )
    spans = call(
        functools.partial(pack_span, outer, inner, rows, span_lines),
        [shape((span_lines + 8, HEAD_DIM))] * outer,
        (token, cache_lengths, new_keys, new_values, queries, expert_ids, expert_weights),
        [pltpu.VMEM((span_lines + 8, HEAD_DIM), f32), pltpu.VMEM((24, top), f32)],
    )
    spans = exchange(outward, spans)
    caches = call(
        functools.partial(pack_cache, outer, inner),
        [shape((2 * cache, HEAD_DIM))] * outer,
        (cache_keys, cache_values),
    )
    caches = exchange(outward, caches)
    wanted = call(
        functools.partial(collect, outer, rows, span_lines),
        shape((asked_lines, HEAD_DIM)),
        spans,
        [pltpu.VMEM((asked_lines, HEAD_DIM), f32)],
    )
    wanted = exchange(inward, [wanted] * inner)

    chunks = call(
        functools.partial(attend, outer, inner, rows, span_lines, count, heads, step),
        [shape((stat_lines(heads * count)[-1][2] + 16, HEAD_DIM))] * inner,
        (pick, *spans, *caches, *wanted),
        [
            pltpu.VMEM((outer * span_lines, HEAD_DIM), f32),
            pltpu.VMEM((GROUP * count, 2 * HEAD_DIM), bf16),
        ],
        grant=max(8, count // 6),
    )
    chunks = exchange(inward, chunks)

    if step < HEAD_DIM:
        at = lax.rem(lax.axis_index("ctx") * step, HEAD_DIM)
        out_weight = lax.dynamic_update_slice(
            jnp.zeros((HEAD_DIM, width), out_weight.dtype), out_weight, (at, 0)
        )
    kept, *parts = call(
        functools.partial(project, inner, rows, count, heads),
        [shape((count, columns), f32)] + [shape((count, columns))] * (inner - 1),
        (*chunks, out_weight, residual_in),
        [pltpu.VMEM((count, width), f32)],
        grant=max(4, count // 12),
    )
    parts = exchange(inward, [None] + parts)[1:]
    both = [shape((count, columns), f32), shape((count, columns))]
    kept, sent = call(add_up, both, (kept, *parts))
    k = 1
    while k < outer:
        kept, sent = call(add_up, both, (kept, outward(sent, k)))
        k *= 2
    pieces = [kept] + exchange(inward, [sent] * inner)[1:]

    weights = call(
        functools.partial(route, outer, inner, rows, count, top),
        shape((count, LANES), f32),
        wanted,
        flops=10**7,
    )
    early = min(2, inner)
    hidden = shape((count, expert_gate.shape[2]), f32)
    gain = norm_gain.reshape(1, width)
    begun = call(
        functools.partial(begin, inner),
        [hidden, hidden, shape((count, LANES), f32)],
        (expert_gate, expert_up, gain, *pieces[:early]),
    )
    kept, sent, state = call(
        functools.partial(expert, inner, early, rows),
        [shape((half, width), f32), shape((half, width)), shape((rows, width), f32)],
        (expert_gate, expert_up, expert_down, gain, weights, *begun, *pieces),
        [pltpu.VMEM((count, width), f32), pltpu.VMEM((count, width), f32)],
        grant=max(8, count // 6),
    )
    sums = call(
        functools.partial(join, rows),
        shape((shards // 2, lines, LANES)),
        (kept, inward(sent, 1)),
        [pltpu.VMEM((half, width), f32), pltpu.VMEM((shards // 2, lines, LANES), f32)],
        grant=max(4, count // 12),
    )
    parity = [[2 * t + odd for t in range(shards // 2)] for odd in range(2)]
    back = lax.all_to_all(
        sums, "ctx", split_axis=0, concat_axis=0, tiled=True, axis_index_groups=parity
    )
    return call(
        functools.partial(combine, rows),
        shape((rows, width)),
        (state, back),
        [pltpu.VMEM((lines, LANES), f32)],
    )


def solution(mesh):
    placed = (
        P(("groups", "ctx"), None),
        P(("groups", "ctx"), None),
        P(("groups", "ctx"), None),
        P(("groups", "ctx"), None),
        P(("groups", "ctx"), None),
        P(("groups", "ctx")),
        P(("groups", "ctx"), None),
        P("ctx", None),
        P(),
        P("ctx", None, None),
        P("ctx", None, None),
        P("ctx", None, None),
        P(("groups", "ctx"), None),
        P(("groups", "ctx"), None),
    )
    return jax.shard_map(
        local, mesh=mesh, in_specs=placed, out_specs=P(("groups", "ctx"), None), check_vma=False
    )
```

```python
import functools

import jax
import jax.numpy as jnp
from jax import lax
from jax.experimental import pallas as pl
from jax.experimental.pallas import tpu as pltpu
from jax.sharding import PartitionSpec as P


HEADS = 32
KV_HEADS = 4
HEAD_DIM = 128
GROUP = HEADS // KV_HEADS
LANES = 128

MASKED = -1e30
epsilon = 1e-06

f32, bf16 = jnp.float32, jnp.bfloat16
VMEM = pl.BlockSpec(memory_space=pltpu.VMEM)


def coordinates(inner):
    device = lax.axis_index("ctx")
    return device // inner, lax.rem(device, inner)


def call(body, outs, operands, scratch=(), grant=4, flops=10**9):
    return pl.pallas_call(
        body,
        out_shape=outs,
        in_specs=[VMEM] * len(operands),
        out_specs=jax.tree.map(lambda _: VMEM, outs),
        scratch_shapes=list(scratch),
        compiler_params=pltpu.CompilerParams(vmem_limit_bytes=grant << 20),
        cost_estimate=pl.CostEstimate(flops=flops, bytes_accessed=10**6, transcendentals=0),
    )(*operands)


def third(x, rows):
    return jnp.right_shift(x * (-(-65536 // rows)), 16)


def owners(position, outer, inner, rows):
    b = third(position, outer * rows)
    rest = position - b * (outer * rows)
    a = third(rest, rows)
    return a * inner + b, rest - a * rows


def place(shard, outer, inner, rows):
    return (lax.rem(shard, inner) * outer + shard // inner) * rows


def stat_lines(lines):
    starts = range(0, lines, LANES)
    return [(s, min(LANES, lines - s), lines + 16 * i) for i, s in enumerate(starts)]


def selection():
    line = lax.broadcasted_iota(jnp.int32, (16, LANES), 0)
    lane = lax.broadcasted_iota(jnp.int32, (16, LANES), 1)
    return jnp.where(line == lane, 1.0, 0.0).astype(bf16)


def aligned(index, size):
    return pl.ds(pl.multiple_of(index * size, size), size)


def pack_span(outer, inner, rows, lines, token, lengths, new_keys, new_values, queries, ids, weights, *refs):
    outs, (wide, routing) = refs[:outer], refs[outer:]
    a, _ = coordinates(inner)
    per_row = rows * GROUP
    live = lengths[...].astype(f32).reshape(1, 1)
    wide[...] = jnp.zeros_like(wide)
    wide[per_row + 2 * rows : per_row + 2 * rows + 1] = jnp.broadcast_to(live, (1, HEAD_DIM))
    weight = weights[...]
    high = weight.astype(bf16).astype(f32)
    routing[...] = jnp.zeros_like(routing)
    for i, part in enumerate((ids[...].astype(f32), high, weight - high)):
        routing[8 * i : 8 * i + rows] = part
    top = ids.shape[1]
    lane = lax.broadcasted_iota(jnp.int32, (top, HEAD_DIM), 1)
    turn = lax.broadcasted_iota(jnp.int32, (top, HEAD_DIM), 0)
    copies = jnp.where(lax.rem(lane, top) == turn, 1.0, 0.0).astype(bf16)
    repeated = jnp.dot(routing[...].astype(bf16), copies, preferred_element_type=f32)
    lane = lax.broadcasted_iota(jnp.int32, (8, HEAD_DIM), 1)
    row = lax.broadcasted_iota(jnp.int32, (8, HEAD_DIM), 0)
    inside = (lane >= row * top) & (lane < row * top + top)
    for i in range(3):
        wide[lines + i : lines + i + 1] = jnp.sum(
            jnp.where(inside, repeated[8 * i : 8 * i + 8], 0.0), axis=0, keepdims=True
        )
    for k in range(outer):
        head = jnp.bitwise_xor(a, k)
        lanes = aligned(head, HEAD_DIM)
        block = queries[:, aligned(head, GROUP * HEAD_DIM)].astype(f32)
        for g in range(GROUP):
            wide[g * rows : (g + 1) * rows] = block[:, g * HEAD_DIM : (g + 1) * HEAD_DIM]
        wide[per_row : per_row + rows] = new_keys[:, lanes].astype(f32)
        wide[per_row + rows : per_row + 2 * rows] = new_values[:, lanes].astype(f32)
        outs[k][...] = wide[...].astype(bf16)


def pack_cache(outer, inner, keys, values, *outs):
    a, _ = coordinates(inner)
    cache = keys.shape[0]
    for k in range(outer):
        lanes = aligned(jnp.bitwise_xor(a, k), HEAD_DIM)
        outs[k][0:cache] = keys[:, lanes]
        outs[k][cache:] = values[:, lanes]


def plan(outer, inner, rows, count, pick, token):
    a, b = coordinates(inner)
    per_row = rows * GROUP
    position = lax.broadcasted_iota(jnp.int32, (count, 1), 0)
    owner, row = owners(position, outer, inner, rows)
    at_a = jnp.bitwise_xor(jnp.right_shift(owner, inner.bit_length() - 1), a)
    at_b = jnp.bitwise_xor(jnp.bitwise_and(owner, inner - 1), b)
    source = (at_b * outer + at_a) * per_row + row
    source = jnp.where(owner < outer * inner, source, -per_row)
    column = lax.broadcasted_iota(jnp.int32, (count, pick.shape[1]), 1)
    for g in range(GROUP):
        pick[g * count : (g + 1) * count] = jnp.where(
            column == source + g * rows, 1.0, 0.0
        ).astype(bf16)
    token[...] = jnp.zeros_like(token)


def collect(outer, rows, lines, *refs):
    spans, out, wide = refs[:outer], refs[outer], refs[outer + 1]
    per_row = rows * GROUP
    for k in range(outer):
        block = spans[k][...].astype(f32)
        wide[k * per_row : (k + 1) * per_row] = block[0:per_row]
        for i in range(3):
            at = outer * per_row + i * outer + k
            wide[at : at + 1] = block[lines + i : lines + i + 1]
    out[...] = wide[...].astype(bf16)


def attend(outer, inner, rows, lines, count, heads, step, *refs):
    pick, spans, caches = refs[0], refs[1 : outer + 1], refs[outer + 1 : 2 * outer + 1]
    queries, refs = refs[2 * outer + 1 : 2 * outer + 1 + inner], refs[2 * outer + 1 + inner :]
    outs, (fresh, parts) = refs[:inner], refs[inner:]
    a, b = coordinates(inner)
    cache = caches[0].shape[0] // 2
    per_row = rows * GROUP
    gathered = jnp.concatenate([block[0 : outer * per_row] for block in queries], 0)
    wanted = jnp.dot(pick[...], gathered, preferred_element_type=f32).astype(bf16)

    def score(keys, usable):
        s = lax.dot_general(
            wanted, keys, (((1,), (1,)), ((), ())), preferred_element_type=f32
        ) * HEAD_DIM ** (-0.5)
        return jnp.where(usable, s.reshape((GROUP, count, keys.shape[0])), MASKED)

    fresh[...] = jnp.zeros_like(fresh)
    owner, row = owners(
        lax.broadcasted_iota(jnp.int32, (count, 1), 0), outer, inner, rows
    )
    position = owner * rows + row
    slot = lax.broadcasted_iota(jnp.int32, (count, outer * lines), 1)
    reach = jnp.full((count, outer * lines), -1, jnp.int32)
    lives = []
    for k in range(outer):
        block = spans[k][0:lines].astype(f32)
        lives.append(block[per_row + 2 * rows : per_row + 2 * rows + 1, 0:1])
        first = k * lines + per_row
        fresh[first : first + rows] = block[per_row + rows : per_row + 2 * rows]
        start = rows * (jnp.bitwise_xor(a, k) * inner + b)
        inside = (slot >= first) & (slot < first + rows)
        reach = jnp.where(inside, position - start - (slot - first), reach)
    keys = [jnp.concatenate([block[0:lines] for block in spans], 0)]
    values = [fresh[...].astype(bf16)]
    usable = [(reach >= 0)[None]]
    index = lax.broadcasted_iota(jnp.int32, (count, cache), 1).astype(f32)
    for k in range(outer):
        keys.append(caches[k][0:cache])
        values.append(caches[k][cache:])
        usable.append(((lives[k] - index) > 0.0)[None])
    scores = [score(key, ok) for key, ok in zip(keys, usable)]
    largest = functools.reduce(
        jnp.maximum, [jnp.max(s, axis=-1, keepdims=True) for s in scores]
    )
    largest = largest.astype(bf16).astype(f32)
    total = jnp.zeros((GROUP, count, 1), f32)
    summed = jnp.zeros((GROUP * count, HEAD_DIM), f32)
    for s, ok, value in zip(scores, usable, values):
        e = jnp.where(ok, jnp.exp(s - largest), 0.0)
        total = total + jnp.sum(e, axis=-1, keepdims=True)
        summed = summed + jnp.dot(
            e.reshape(GROUP * count, value.shape[0]).astype(bf16),
            value,
            preferred_element_type=f32,
        )
    total = total.reshape(GROUP * count, 1)
    high = total.astype(bf16).astype(f32)
    lane = lax.broadcasted_iota(jnp.int32, (GROUP * count, HEAD_DIM), 1)
    stats = jnp.where(
        lane == 0,
        largest.reshape(GROUP * count, 1),
        jnp.where(lane == 1, high, total - high),
    )
    parts[:, 0:HEAD_DIM] = summed.astype(bf16)
    parts[:, HEAD_DIM:] = stats.astype(bf16)
    for k in range(inner):
        first = jnp.right_shift(jnp.bitwise_xor(b, k) * step, HEAD_DIM.bit_length() - 1)
        first, lines = pl.multiple_of(first * count, 16), heads * count
        outs[k][0:lines] = parts[pl.ds(first, lines), 0:HEAD_DIM]
        outs[k][lines:] = jnp.zeros((outs[k].shape[0] - lines, LANES), bf16)
        for start, size, at in stat_lines(lines):
            block = parts[pl.ds(pl.multiple_of(first + start, 16), size), HEAD_DIM:]
            outs[k][at : at + 16, 0:size] = lax.dot_general(
                selection(), block, (((1,), (1,)), ((), ())), preferred_element_type=f32
            ).astype(bf16)


def project(outer, inner, rows, count, heads, *refs):
    chunks, (weight, residual), refs = refs[:inner], refs[inner : inner + 2], refs[inner + 2 :]
    own, outs, total = refs[0], refs[1:inner], refs[inner]
    _, b = coordinates(inner)
    lines = heads * count
    stats = [
        jnp.concatenate(
            [
                lax.dot_general(
                    chunk[at : at + 16, 0:size],
                    selection(),
                    (((0,), (0,)), ((), ())),
                    preferred_element_type=f32,
                )
                for _, size, at in stat_lines(lines)
            ],
            0,
        )
        for chunk in chunks
    ]
    largest = functools.reduce(jnp.maximum, [s[:, 0:1] for s in stats])
    scales = [jnp.exp(s[:, 0:1] - largest) for s in stats]
    denominator = sum(w * (s[:, 1:2] + s[:, 2:3]) for w, s in zip(scales, stats))
    joined = sum(
        chunk[0:lines].astype(f32) * (w / denominator)
        for w, chunk in zip(scales, chunks)
    ).astype(bf16)
    total[...] = sum(
        jnp.dot(
            joined[h * count : (h + 1) * count],
            weight[h * HEAD_DIM : (h + 1) * HEAD_DIM],
            preferred_element_type=f32,
        )
        for h in range(heads)
    )
    start = place(lax.axis_index("ctx"), outer, inner, rows)
    added = residual[...].astype(f32)
    for r in range(rows):
        row = pl.ds(start + r, 1)
        total[row] = total[row] + added[r : r + 1]
    columns = own.shape[1]
    own[...] = total[:, aligned(b, columns)]
    for k in range(1, inner):
        outs[k - 1][...] = total[:, aligned(jnp.bitwise_xor(b, k), columns)].astype(bf16)


def add_up(own, *refs):
    others, (kept, sent) = refs[:-2], refs[-2:]
    partial = own[...]
    for other in others:
        partial = partial + other[...].astype(f32)
    kept[...] = partial
    sent[...] = partial.astype(bf16)


def route(outer, inner, rows, top, *refs):
    blocks, out = refs[:-1], refs[-1]
    a, b = coordinates(inner)
    out[...] = jnp.zeros_like(out)
    expert = lax.axis_index("ctx").astype(f32)
    lane = lax.broadcasted_iota(jnp.int32, (outer, HEAD_DIM), 1)
    for m in range(inner):
        info = blocks[m][outer * rows * GROUP :].astype(f32)
        named, high, low = (info[i * outer : (i + 1) * outer] for i in range(3))
        weight = jnp.where(named == expert, high + low, 0.0)
        for r in range(rows):
            inside = (lane >= r * top) & (lane < r * top + top)
            share = jnp.sum(jnp.where(inside, weight, 0.0), axis=1, keepdims=True)
            share = jnp.broadcast_to(share, (outer, LANES))
            for k in range(outer):
                shard = jnp.bitwise_xor(a, k) * inner + jnp.bitwise_xor(b, m)
                out[pl.ds(place(shard, outer, inner, rows) + r, 1)] = share[k : k + 1]


def begin(inner, gate, up, gain, *refs):
    pieces, (gated, lifted, squares) = refs[:-3], refs[-3:]
    _, b = coordinates(inner)
    columns = pieces[0].shape[1]
    total, sums = jnp.zeros(squares.shape, f32), [0.0, 0.0]
    for k, piece in enumerate(pieces):
        lanes = aligned(jnp.bitwise_xor(b, k), columns)
        value = piece[...].astype(f32)
        total = total + jnp.sum(value * value, axis=1, keepdims=True)
        x = (value * gain[:, lanes].astype(f32)).astype(bf16)
        for i, weight in enumerate((gate, up)):
            sums[i] = sums[i] + jnp.dot(x, weight[0, lanes], preferred_element_type=f32)
    gated[...], lifted[...] = sums
    squares[...] = total


def expert(
    outer, inner, early, rows, gate, up, down, gain, weights, begun_gate, begun_up, begun, *refs
):
    pieces, refs = refs[:inner], refs[inner:]
    kept, outs, (mine, state, held, dense) = refs[0], refs[1:inner], refs[inner:]
    _, b = coordinates(inner)
    columns = pieces[0].shape[1]
    squares, gated, lifted = begun[:, 0:1], begun_gate[...], begun_up[...]
    for k, piece in enumerate(pieces):
        lanes = aligned(jnp.bitwise_xor(b, k), columns)
        value = piece[...].astype(f32)
        state[:, lanes] = value
        if k >= early:
            squares = squares + jnp.sum(value * value, axis=1, keepdims=True)
            x = (value * gain[:, lanes].astype(f32)).astype(bf16)
            gated = gated + jnp.dot(x, gate[0, lanes], preferred_element_type=f32)
            lifted = lifted + jnp.dot(x, up[0, lanes], preferred_element_type=f32)
    scale = lax.rsqrt(squares * (1.0 / (inner * columns)) + epsilon)
    gated, lifted = gated * scale, lifted * scale
    start = place(lax.axis_index("ctx"), outer, inner, rows)
    for r in range(rows):
        mine[r : r + 1] = state[pl.ds(start + r, 1)]
    active = (gated / (1.0 + jnp.exp(-gated)) * lifted).astype(bf16)
    held[...] = jnp.dot(active, down[0], preferred_element_type=f32) * weights[:, 0:1]
    block = outer * rows
    for m in range(inner):
        for j in range(held.shape[1] // LANES):
            dense[m, j * block : (j + 1) * block] = held[
                m * block : (m + 1) * block, j * LANES : (j + 1) * LANES
            ]
    kept[...] = dense[b]
    for k in range(1, inner):
        outs[k - 1][...] = dense[jnp.bitwise_xor(b, k)].astype(bf16)


def join(outer, inner, rows, *refs):
    kept, others, refs = refs[0], refs[1:inner], refs[inner:]
    own, outs, (total, dense) = refs[0], refs[1:outer], refs[outer:]
    a, _ = coordinates(inner)
    total[...] = functools.reduce(lambda x, y: x + y[...].astype(f32), others, kept[...])
    block = outer * rows
    for t in range(outer):
        for j in range(total.shape[0] // block):
            at = j * block + t * rows
            dense[t, j * rows : (j + 1) * rows] = total[at : at + rows]
    own[...] = dense[a]
    for k in range(1, outer):
        outs[k - 1][...] = dense[jnp.bitwise_xor(a, k)].astype(bf16)


def combine(rows, state, own, *refs):
    others, (out, total) = refs[:-2], refs[-2:]
    total[...] = functools.reduce(lambda x, y: x + y[...].astype(f32), others, own[...])
    for j in range(state.shape[1] // LANES):
        lanes = slice(j * LANES, (j + 1) * LANES)
        out[:, lanes] = (state[:, lanes] + total[j * rows : (j + 1) * rows]).astype(bf16)


def local(
    queries,
    cache_keys,
    cache_values,
    new_keys,
    new_values,
    cache_lengths,
    residual_in,
    out_weight,
    norm_gain,
    expert_gate,
    expert_up,
    expert_down,
    expert_ids,
    expert_weights,
):
    shards = lax.axis_size("ctx")
    outer = KV_HEADS
    inner = shards // outer
    rows, width = residual_in.shape
    cache = cache_keys.shape[0]
    count = -(-shards * rows // 16) * 16
    top = expert_ids.shape[1]
    step = out_weight.shape[0]
    heads = max(1, step // HEAD_DIM)
    columns = width // inner
    lines = rows * width // LANES

    def shape(dims, dtype=bf16):
        return jax.ShapeDtypeStruct(dims, dtype)

    def outward(x, k):
        pairs = [(i, ((i // inner) ^ k) * inner + i % inner) for i in range(shards)]
        return lax.ppermute(x, "ctx", pairs)

    def inward(x, k):
        pairs = [(i, i // inner * inner + ((i % inner) ^ k)) for i in range(shards)]
        return lax.ppermute(x, "ctx", pairs)

    def exchange(move, blocks):
        moved = [blocks[0]]
        for k in range(1, len(blocks)):
            moved.append(move(blocks[k], k))
        return moved

    per_row = rows * GROUP
    span_lines = -(-(per_row + 2 * rows + 1) // 16) * 16
    asked_lines = outer * per_row + -(-3 * outer // 8) * 8
    pick, token = call(
        functools.partial(plan, outer, inner, rows, count),
        [shape((GROUP * count, shards * per_row)), shape((8, LANES), f32)],
        (),
        grant=max(4, count // 12),
    )
    spans = call(
        functools.partial(pack_span, outer, inner, rows, span_lines),
        [shape((span_lines + 8, HEAD_DIM))] * outer,
        (token, cache_lengths, new_keys, new_values, queries, expert_ids, expert_weights),
        [pltpu.VMEM((span_lines + 8, HEAD_DIM), f32), pltpu.VMEM((24, top), f32)],
    )
    spans = exchange(outward, spans)
    caches = call(
        functools.partial(pack_cache, outer, inner),
        [shape((2 * cache, HEAD_DIM))] * outer,
        (cache_keys, cache_values),
    )
    caches = exchange(outward, caches)
    wanted = call(
        functools.partial(collect, outer, rows, span_lines),
        shape((asked_lines, HEAD_DIM)),
        spans,
        [pltpu.VMEM((asked_lines, HEAD_DIM), f32)],
    )
    wanted = exchange(inward, [wanted] * inner)

    chunks = call(
        functools.partial(attend, outer, inner, rows, span_lines, count, heads, step),
        [shape((stat_lines(heads * count)[-1][2] + 16, HEAD_DIM))] * inner,
        (pick, *spans, *caches, *wanted),
        [
            pltpu.VMEM((outer * span_lines, HEAD_DIM), f32),
            pltpu.VMEM((GROUP * count, 2 * HEAD_DIM), bf16),
        ],
        grant=max(8, count // 6),
    )
    chunks = exchange(inward, chunks)

    if step < HEAD_DIM:
        at = lax.rem(lax.axis_index("ctx") * step, HEAD_DIM)
        out_weight = lax.dynamic_update_slice(
            jnp.zeros((HEAD_DIM, width), out_weight.dtype), out_weight, (at, 0)
        )
    kept, *parts = call(
        functools.partial(project, outer, inner, rows, count, heads),
        [shape((count, columns), f32)] + [shape((count, columns))] * (inner - 1),
        (*chunks, out_weight, residual_in),
        [pltpu.VMEM((count, width), f32)],
        grant=max(4, count // 12),
    )
    parts = exchange(inward, [None] + parts)[1:]
    both = [shape((count, columns), f32), shape((count, columns))]
    kept, sent = call(add_up, both, (kept, *parts))
    k = 1
    while k < outer:
        kept, sent = call(add_up, both, (kept, outward(sent, k)))
        k *= 2
    pieces = [kept] + exchange(inward, [sent] * inner)[1:]

    weights = call(
        functools.partial(route, outer, inner, rows, top),
        shape((count, LANES), f32),
        wanted,
        flops=10**7,
    )
    early = min(2, inner)
    hidden = shape((count, expert_gate.shape[2]), f32)
    gain = norm_gain.reshape(1, width)
    begun = call(
        functools.partial(begin, inner),
        [hidden, hidden, shape((count, LANES), f32)],
        (expert_gate, expert_up, gain, *pieces[:early]),
    )
    gathered = (outer * lines, LANES)
    kept, *rest = call(
        functools.partial(expert, outer, inner, early, rows),
        [shape(gathered, f32)]
        + [shape(gathered)] * (inner - 1)
        + [shape((rows, width), f32)],
        (expert_gate, expert_up, expert_down, gain, weights, *begun, *pieces),
        [
            pltpu.VMEM((count, width), f32),
            pltpu.VMEM((count, width), f32),
            pltpu.VMEM((inner,) + gathered, f32),
        ],
        grant=max(8, count // 6),
    )
    state = rest.pop()
    others = exchange(inward, [None] + rest)[1:]
    own, *rest = call(
        functools.partial(join, outer, inner, rows),
        [shape((lines, LANES), f32)] + [shape((lines, LANES))] * (outer - 1),
        (kept, *others),
        [pltpu.VMEM(gathered, f32), pltpu.VMEM((outer, lines, LANES), f32)],
    )
    others = exchange(outward, [None] + rest)[1:]
    return call(
        functools.partial(combine, rows),
        shape((rows, width)),
        (state, own, *others),
        [pltpu.VMEM((lines, LANES), f32)],
    )


def solution(mesh):
    placed = (
        P(("groups", "ctx"), None),
        P(("groups", "ctx"), None),
        P(("groups", "ctx"), None),
        P(("groups", "ctx"), None),
        P(("groups", "ctx"), None),
        P(("groups", "ctx")),
        P(("groups", "ctx"), None),
        P("ctx", None),
        P(),
        P("ctx", None, None),
        P("ctx", None, None),
        P("ctx", None, None),
        P(("groups", "ctx"), None),
        P(("groups", "ctx"), None),
    )
    return jax.shard_map(
        local, mesh=mesh, in_specs=placed, out_specs=P(("groups", "ctx"), None), check_vma=False
    )
```
